32 devices in a mesh: blk: 8 (over y, x, core), grp: 4 (over z).
Axes of the slice: x: 2, y: 2, z: 4, core: 2. Of those that a mesh axis runs over, the one named last changes fastest.
Arguments:
- source_rows: float32 [8, 4, 400, 768], P('blk', 'grp'), may hold values from -2.4 to 2.4
- source_state: float32 [8, 4, 768], P('blk', 'grp'), may hold values from 0.05 to 1
- target_rows: float32 [8, 4, 400, 512], P('blk', 'grp'), may hold values from -12.5 to 12.5
- destination_state: float32 [8, 4, 512], P('blk', 'grp'), may hold values from 0.05 to 1
- positives: int32 [4, 8, 4, 768], P(None, 'blk', 'grp'), may hold values from 0 to 511
- relation_ids: int32 [4, 8, 4], P(None, 'blk', 'grp'), may hold values from 0 to 1
- relations: float32 [2, 400, 400], replicated, may hold values from -0.36 to 1.36
Outputs:
- source_out: float32 [8, 4, 400, 768], P('blk', 'grp')
- source_state_out: float32 [8, 4, 768], P('blk', 'grp')
- target_out: float32 [8, 4, 400, 512], P('blk', 'grp')
- target_state_out: float32 [8, 4, 512], P('blk', 'grp')
- relations_out: float32 [2, 400, 400], replicated
- operator_grads: float32 [2, 2, 400, 400], replicated
The draws below stay inside these ranges and needn't reach their ends.
All inputs are finite; a program needn't handle non-finite values.
Results may differ from the reference program's by a relative error of at most 0.0003.
Values sent between devices are 32-bit elements; how exact they have to be, the bound alone decides.
No kernel may reach another device: no remote copies, remote signals or barrier semaphores. Data moves between devices by JAX's collectives and lax.ppermute only.
A program may use at most 64 MiB of HBM per device.

```python
import math
import jax
import jax.numpy as jnp
from jax import lax

EMBED_WIDTH = 400
SOURCE_DEV_ROWS = 768
DEST_BLOCK_ROWS = 512
STEPS = 4
NREL = 2
N_BLK = 8
N_GRP = 4


def pair_fields(key):
    base = jax.random.fold_in(key, 11)
    first_key, second_key = jax.random.split(base)
    source_block = jnp.clip(0.4 * jax.random.normal(first_key, (N_BLK, N_GRP, EMBED_WIDTH, SOURCE_DEV_ROWS), jnp.float32), -2.4, 2.4)
    target_block = jnp.clip(0.4 * jax.random.normal(second_key, (N_BLK, N_GRP, EMBED_WIDTH, DEST_BLOCK_ROWS), jnp.float32), -2.4, 2.4)
    return (source_block, target_block)


def draw_source_rows(key, part):
    return pair_fields(key)[0]


def draw_target_rows(key, part):
    return pair_fields(key)[1]


def draw_relations(key, part):
    noise = jnp.clip(jax.random.normal(jax.random.fold_in(key, 23), (NREL, EMBED_WIDTH, EMBED_WIDTH), jnp.float32), -4.0, 4.0)
    return jnp.eye(EMBED_WIDTH, dtype=jnp.float32)[None] + 0.5 / math.sqrt(EMBED_WIDTH) * noise


def place_ends(array, key, smallest, largest):
    index_at = [jax.random.randint(jax.random.fold_in(key, axis), (), 0, length) for axis, length in enumerate(array.shape)]
    main_axis = array.shape.index(max(array.shape))
    next_to = index_at[:main_axis] + [(index_at[main_axis] + 1) % array.shape[main_axis]] + index_at[main_axis + 1:]
    return array.at[tuple(index_at)].set(smallest).at[tuple(next_to)].set(largest)


def level_of(own_key, dims, cuts, least, top_value):
    gain, own = 1.0, jax.random.fold_in(own_key, 6)
    for position, shards_of in cuts:
        steps = jnp.exp(jax.random.uniform(jax.random.fold_in(own, position), (shards_of,), jnp.float32, least / len(cuts), top_value / len(cuts)))
        gain = gain * jnp.repeat(steps, dims[position] // shards_of).reshape([-1 if axis == position else 1 for axis in range(len(dims))])
    return gain


def setup_inputs(seed: int = 0) -> dict:
    seeds = jax.random.split(jax.random.key(seed), 8)
    return {
        "source_rows": draw_source_rows(jax.random.fold_in(seeds[7], 71), 0),
        "source_state": jnp.clip(jnp.exp(math.log(1.0) - 2.9957323 * jax.random.uniform(seeds[1], (N_BLK, N_GRP, SOURCE_DEV_ROWS), jnp.float32) ** level_of(seeds[1], (N_BLK, N_GRP, SOURCE_DEV_ROWS), ((0, 8), (1, 4)), -0.2, 0.2)), 0.05, 1.0),
        "target_rows": draw_target_rows(jax.random.fold_in(seeds[7], 71), 0),
        "destination_state": jnp.clip(jnp.exp(math.log(1.0) - 2.9957323 * jax.random.uniform(seeds[3], (N_BLK, N_GRP, DEST_BLOCK_ROWS), jnp.float32) ** level_of(seeds[3], (N_BLK, N_GRP, DEST_BLOCK_ROWS), ((0, 8), (1, 4)), -0.2, 0.2)), 0.05, 1.0),
        "positives": place_ends(jax.random.randint(seeds[4], (STEPS, N_BLK, N_GRP, SOURCE_DEV_ROWS), 0, DEST_BLOCK_ROWS), jax.random.fold_in(seeds[4], 1), 0, DEST_BLOCK_ROWS - 1).astype(jnp.int32),
        "relation_ids": place_ends(jax.random.randint(seeds[5], (STEPS, N_BLK, N_GRP), 0, NREL), jax.random.fold_in(seeds[5], 1), 0, NREL - 1).astype(jnp.int32),
        "relations": draw_relations(jax.random.fold_in(seeds[7], 71), 0),
    }


entity_rate = 0.1
operator_rate = 0.01
grad_gain = 6.0

def highest_dot(left, right):
    return jnp.dot(left, right, precision=lax.Precision.HIGHEST, preferred_element_type=jnp.float32)

def adagrad_rows(values, state, gradient):
    state_new = state + lax.optimization_barrier(jnp.mean(gradient * gradient, axis=0))
    return (values - entity_rate * gradient / jnp.sqrt(state_new)[None, :], state_new)

def apply_bucket_step(source_block, source_state, target_block, destination_state, partner, relation_matrix):
    queries = highest_dot(relation_matrix.T, source_block)
    scores = highest_dot(queries.T, target_block)
    highest = lax.optimization_barrier(jnp.max(scores, axis=1, keepdims=True))
    expo = jnp.exp(scores - highest)
    chance = expo / lax.optimization_barrier(jnp.sum(expo, axis=1, keepdims=True))
    columns = jnp.arange(target_block.shape[1], dtype=jnp.int32)
    onehot = (columns[None, :] == partner[:, None]).astype(jnp.float32)
    score_grad = chance - onehot
    target_grad = highest_dot(queries, score_grad)
    query_grad = highest_dot(target_block, score_grad.T)
    source_grad = highest_dot(relation_matrix, query_grad)
    relation_matrix_gradient = highest_dot(source_block, query_grad.T)
    source_new, source_state_new = adagrad_rows(source_block, source_state, source_grad)
    target_new, target_state_new = adagrad_rows(target_block, destination_state, target_grad)
    return (source_new, source_state_new, target_new, target_state_new, relation_matrix_gradient)

def reference(source_rows, source_state, target_rows, destination_state, positives, relation_ids, relations):
    hit_count = N_BLK * N_GRP
    gradient_scale = grad_gain / jnp.sqrt(jnp.float32(SOURCE_DEV_ROWS * hit_count))
    source_block = source_rows.reshape(hit_count, EMBED_WIDTH, SOURCE_DEV_ROWS)
    source_block_state = source_state.reshape(hit_count, SOURCE_DEV_ROWS)
    target_block = target_rows
    target_block_state = destination_state
    relation_matrices = relations
    running_totals = jnp.zeros((NREL, EMBED_WIDTH, EMBED_WIDTH), jnp.float32)
    bucket_results = []
    kinds = jnp.arange(NREL, dtype=jnp.int32)
    for bucket_cell in range(STEPS):
        flattened_target = target_block.reshape(hit_count, EMBED_WIDTH, DEST_BLOCK_ROWS)
        flattened_target_state = target_block_state.reshape(hit_count, DEST_BLOCK_ROWS)
        partner_rows = positives[bucket_cell].reshape(hit_count, SOURCE_DEV_ROWS)
        picked_indices = relation_ids[bucket_cell].reshape(hit_count)

        def single_pair(carry, item):
            src_cols, src_state, tgt_cols, tgt_state, partner, relation_index = item
            relation_matrix = relation_matrices[relation_index]
            out = apply_bucket_step(src_cols, src_state, tgt_cols, tgt_state, partner, relation_matrix)
            chosen = (kinds == relation_index).astype(jnp.float32)
            return (carry + chosen[:, None, None] * out[4][None], out[:4])
        running_totals, refreshed_block = lax.scan(single_pair, running_totals, (source_block, source_block_state, flattened_target, flattened_target_state, partner_rows, picked_indices))
        source_block, source_block_state = (refreshed_block[0], refreshed_block[1])
        target_block = jnp.roll(refreshed_block[2].reshape(N_BLK, N_GRP, EMBED_WIDTH, DEST_BLOCK_ROWS), 1, axis=0)
        target_block_state = jnp.roll(refreshed_block[3].reshape(N_BLK, N_GRP, DEST_BLOCK_ROWS), 1, axis=0)
        if bucket_cell % 2 == 1:
            scaled = gradient_scale * running_totals
            bucket_results.append(scaled)
            relation_matrices = relation_matrices - operator_rate * scaled
            running_totals = jnp.zeros((NREL, EMBED_WIDTH, EMBED_WIDTH), jnp.float32)
    return (source_block.reshape(N_BLK, N_GRP, EMBED_WIDTH, SOURCE_DEV_ROWS), source_block_state.reshape(N_BLK, N_GRP, SOURCE_DEV_ROWS), target_block, target_block_state, relation_matrices, jnp.stack(bucket_results))
```

```python
import math

import jax
import jax.numpy as jnp
from jax import lax
from jax.sharding import PartitionSpec as P

entity_rate = 0.1
operator_rate = 0.01
grad_gain = 6.0
AXES = ("blk", "grp")


def from_behind(value, axis, steps):
    count = lax.axis_size(axis)
    pairs = [(source, (source + steps) % count) for source in range(count)]
    return lax.ppermute(value, axis, pairs)


def high_dot(left, right):
    return jnp.dot(left, right, precision=lax.Precision.HIGH, preferred_element_type=jnp.float32)


def exchange(value, blk_mask, grp_mask):
    blk, grp = lax.axis_size("blk"), lax.axis_size("grp")
    pairs = [(b * grp + g, (b ^ blk_mask) * grp + (g ^ grp_mask)) for b in range(blk) for g in range(grp)]
    return lax.ppermute(value, AXES, pairs)


def group_masks(bits):
    masks = []
    for member in range(1, 1 << len(bits)):
        blk_mask = sum(m for i, (axis, m) in enumerate(bits) if axis == "blk" and member >> i & 1)
        grp_mask = sum(m for i, (axis, m) in enumerate(bits) if axis == "grp" and member >> i & 1)
        masks.append((member, blk_mask, grp_mask))
    return sorted(masks, key=lambda t: -bin(t[0]).count("1"))


def own_member(bits):
    member = 0
    for i, (axis, m) in enumerate(bits):
        member = member + (((lax.axis_index(axis) // m) % 2) << i)
    return member


def take(blocks, index):
    return lax.dynamic_index_in_dim(blocks, index, 0, keepdims=False)


def scatter_sum(value, bits):
    blocks = value.reshape((1 << len(bits), -1) + value.shape[1:])
    me = own_member(bits)
    total = take(blocks, me)
    arrived = [exchange(take(blocks, me ^ d), mb, mg) for d, mb, mg in group_masks(bits)]
    for block in arrived:
        total = total + block
    return total


def gather(value, bits):
    arrived = {d: exchange(value, mb, mg) for d, mb, mg in group_masks(bits)}
    arrived[0] = value
    me = own_member(bits)
    blocks = jnp.stack([arrived[d] for d in range(1 << len(bits))])
    ordered = jnp.stack([take(blocks, me ^ d) for d in range(1 << len(bits))])
    return ordered.reshape((-1,) + value.shape[1:])


def sum_everywhere(value):
    blk, grp = lax.axis_size("blk"), lax.axis_size("grp")
    if blk & (blk - 1) or grp & (grp - 1):
        return lax.psum(value, AXES)
    bits = [("blk", 1 << i) for i in range(blk.bit_length() - 1)], [("grp", 1 << i) for i in range(grp.bit_length() - 1)]
    stages = [bits[0][:1], bits[0][1:3], bits[1][:1]]
    for stage in stages:
        value = scatter_sum(value, stage)
    for axis, mask in bits[0][3:] + bits[1][1:]:
        value = value + exchange(value, mask if axis == "blk" else 0, mask if axis == "grp" else 0)
    for stage in reversed(stages):
        value = gather(value, stage)
    return value


def reduce_grads(running_totals):
    kinds, width = running_totals.shape[0], running_totals.shape[1]
    rows = -(-kinds * width // 128) * 128
    flat = jnp.pad(running_totals.reshape(kinds * width, width), ((0, rows - kinds * width), (0, 0)))
    return sum_everywhere(flat)[: kinds * width].reshape(running_totals.shape)


def adagrad_rows(values, state, gradient):
    state_new = state + jnp.mean(gradient * gradient, axis=0)
    return (values - entity_rate * gradient / jnp.sqrt(state_new)[None, :], state_new)


def apply_bucket_step(source_block, source_state, target_block, destination_state, partner, relation_matrix):
    queries = high_dot(relation_matrix.T, source_block)
    scores = high_dot(queries.T, target_block)
    highest = jnp.max(scores, axis=1, keepdims=True)
    expo = jnp.exp(scores - highest)
    chance = expo / jnp.sum(expo, axis=1, keepdims=True)
    columns = jnp.arange(target_block.shape[1], dtype=jnp.int32)
    onehot = (columns[None, :] == partner[:, None]).astype(jnp.float32)
    score_grad = chance - onehot
    target_grad = high_dot(queries, score_grad)
    query_grad = high_dot(target_block, score_grad.T)
    source_grad = high_dot(relation_matrix, query_grad)
    relation_matrix_gradient = high_dot(source_block, query_grad.T)
    source_new, source_state_new = adagrad_rows(source_block, source_state, source_grad)
    target_new, target_state_new = adagrad_rows(target_block, destination_state, target_grad)
    return (source_new, source_state_new, target_new, target_state_new, relation_matrix_gradient)


def shards(source_rows, source_state, target_rows, destination_state, positives, relation_ids, relations):
    source_block = source_rows[0, 0]
    source_block_state = source_state[0, 0]
    target_block = target_rows[0, 0]
    target_block_state = destination_state[0, 0]
    relation_matrices = relations
    kinds_count = relations.shape[0]
    width = relations.shape[1]
    everyone = source_block.shape[1] * lax.axis_size("blk") * lax.axis_size("grp")
    gradient_scale = grad_gain / math.sqrt(everyone)
    kinds = jnp.arange(kinds_count, dtype=jnp.int32)
    running_totals = jnp.zeros((kinds_count, width, width), jnp.float32)
    bucket_results = []
    for bucket_cell in range(positives.shape[0]):
        relation_index = relation_ids[bucket_cell, 0, 0]
        chosen = (kinds == relation_index).astype(jnp.float32)
        relation_matrix = jnp.sum(chosen[:, None, None] * relation_matrices, axis=0)
        (
            source_block,
            source_block_state,
            target_block,
            target_block_state,
            relation_matrix_gradient,
        ) = apply_bucket_step(
            source_block,
            source_block_state,
            target_block,
            target_block_state,
            positives[bucket_cell, 0, 0],
            relation_matrix,
        )
        running_totals = running_totals + chosen[:, None, None] * relation_matrix_gradient[None]
        target_block, target_block_state = from_behind((target_block, target_block_state), "blk", 1)
        if bucket_cell % 2 == 1:
            scaled = gradient_scale * reduce_grads(running_totals)
            bucket_results.append(scaled)
            relation_matrices = relation_matrices - operator_rate * scaled
            running_totals = jnp.zeros((kinds_count, width, width), jnp.float32)
    return (
        source_block[None, None],
        source_block_state[None, None],
        target_block[None, None],
        target_block_state[None, None],
        relation_matrices,
        jnp.stack(bucket_results),
    )


def solution(mesh):
    rows, columns = P("blk", "grp", None, None), P("blk", "grp", None)
    in_specs = (rows, columns, rows, columns, P(None, "blk", "grp", None), P(None, "blk", "grp"), P())
    out_specs = (rows, columns, rows, columns, P(), P())
    return jax.shard_map(shards, mesh=mesh, in_specs=in_specs, out_specs=out_specs, check_vma=False)
```

```python
import functools
import math

import jax
import jax.numpy as jnp
from jax import lax
from jax.experimental import pallas as pl
from jax.experimental.pallas import tpu as pltpu
from jax.sharding import PartitionSpec as P

entity_rate = 0.1
operator_rate = 0.01
grad_gain = 6.0
AXES = ("blk", "grp")
LANES = 128
F32, BF16 = jnp.float32, jnp.bfloat16


def round_up(value, step):
    return -(-value // step) * step


def from_behind(value, axis, steps):
    count = lax.axis_size(axis)
    pairs = [(source, (source + steps) % count) for source in range(count)]
    return lax.ppermute(value, axis, pairs)


def exchange(value, blk_mask, grp_mask):
    blk, grp = lax.axis_size("blk"), lax.axis_size("grp")
    pairs = [(b * grp + g, (b ^ blk_mask) * grp + (g ^ grp_mask)) for b in range(blk) for g in range(grp)]
    return lax.ppermute(value, AXES, pairs)


def group_masks(bits):
    masks = []
    for member in range(1, 1 << len(bits)):
        blk_mask = sum(m for i, (axis, m) in enumerate(bits) if axis == "blk" and member >> i & 1)
        grp_mask = sum(m for i, (axis, m) in enumerate(bits) if axis == "grp" and member >> i & 1)
        masks.append((member, blk_mask, grp_mask))
    return sorted(masks, key=lambda t: -bin(t[0]).count("1"))


def own_member(bits):
    member = jnp.int32(0)
    for i, (axis, m) in enumerate(bits):
        member = member + (((lax.axis_index(axis) // m) % 2) << i)
    return member


def reduce_plan(blk, grp):
    if blk & (blk - 1) or grp & (grp - 1):
        return None
    blk_bits = [("blk", 1 << i) for i in range(blk.bit_length() - 1)]
    grp_bits = [("grp", 1 << i) for i in range(grp.bit_length() - 1)]
    stages = [s for s in (blk_bits[:1], blk_bits[1:3], grp_bits[:1]) if s]
    return (stages, blk_bits[3:] + grp_bits[1:]) if len(stages) > 1 else None


def scatter_sum(value, bits):
    blocks = value.reshape((1 << len(bits), -1) + value.shape[1:])
    total = blocks[0]
    for block in [exchange(blocks[d], mb, mg) for d, mb, mg in group_masks(bits)]:
        total = total + block
    return total


def gather(value, bits):
    arrived = {d: exchange(value, mb, mg) for d, mb, mg in group_masks(bits)}
    arrived[0] = value
    return jnp.concatenate([arrived[d] for d in range(1 << len(bits))], axis=0)


def piece_plan():
    plan = reduce_plan(lax.axis_size("blk"), lax.axis_size("grp"))
    if plan is None:
        return 1, jnp.int32(0)
    count, me = 1, jnp.int32(0)
    for stage in plan[0]:
        count <<= len(stage)
        me = (me << len(stage)) + own_member(stage)
    return count, me


def sum_everywhere(packed, work, args):
    plan = reduce_plan(lax.axis_size("blk"), lax.axis_size("grp"))
    if plan is None:
        after, *rest = work(*args)
        return lax.psum(packed, AXES), from_behind(after, "blk", 1), *rest
    stages, singles = plan
    for place, stage in enumerate(stages):
        if place == 1:
            packed, args = lax.optimization_barrier((packed, args))
            after, *rest = work(*args)
        packed = scatter_sum(packed, stage)
        if place == 1:
            packed, after = lax.optimization_barrier((packed, after))
            arriving = from_behind(after, "blk", 1)
    for axis, mask in singles:
        packed = packed + exchange(packed, mask if axis == "blk" else 0, mask if axis == "grp" else 0)
    for place, stage in reversed(list(enumerate(stages))):
        if place == 1:
            packed, arriving = lax.optimization_barrier((packed, arriving))
        packed = gather(packed, stage)
    return packed, arriving, *rest


NN = (((1,), (0,)), ((), ()))
NT = (((1,), (1,)), ((), ()))


def dot3(ah, al, bh, bl, dims):
    one = functools.partial(lax.dot_general, dimension_numbers=dims, preferred_element_type=F32)
    return one(ah, bh) + (one(ah, bl) + one(al, bh))


def split(x):
    high = x.astype(BF16)
    return high, (x - high.astype(F32)).astype(BF16)


def put_split(refs, x):
    rows = x.shape[0]
    refs[0][:rows], refs[1][:rows] = split(x)
    if rows < refs[0].shape[0]:
        blank = jnp.zeros((refs[0].shape[0] - rows, x.shape[1]), BF16)
        refs[0][rows:], refs[1][rows:] = blank, blank


def both(refs, rows=None):
    return (refs[0][...], refs[1][...]) if rows is None else (refs[0][:rows], refs[1][:rows])


def pad_rows(x, rows):
    return jnp.concatenate([x, jnp.zeros((rows - x.shape[0], x.shape[1]), x.dtype)], axis=0)


def square_of(pad_ref, matrix):
    width = matrix.shape[0]
    pad_ref[...] = jnp.zeros(pad_ref.shape, F32)
    pad_ref[:width, :width] = matrix


def queries_into(q_refs, square_ref, x_refs, width):
    transposed = split(square_ref[...].T[:width])
    put_split(q_refs, dot3(*transposed, *both(x_refs), NN))


def score_grad_into(sg_refs, q_refs, target, partner):
    wide = q_refs[0].shape[0]
    scores = dot3(*split(pad_rows(target, wide).T), *both(q_refs), NN)
    expo = jnp.exp(scores - jnp.max(scores, axis=0, keepdims=True))
    chance = expo * (1.0 / jnp.sum(expo, axis=0, keepdims=True))
    row = lax.broadcasted_iota(jnp.int32, scores.shape, 0)
    put_split(sg_refs, chance - jnp.where(row == partner, 1.0, 0.0))


def adagrad(values, state, gradient):
    state_new = state + jnp.sum(gradient * gradient, axis=0, keepdims=True) * (1.0 / values.shape[0])
    return values - gradient * (entity_rate / jnp.sqrt(state_new)), state_new


def target_into(out_ref, q_refs, sg_refs, target, state):
    width = target.shape[0]
    gradient = dot3(*both(q_refs, width), *both(sg_refs), NT)
    out_ref[:width], out_ref[width : width + 1] = adagrad(target, state, gradient)
    rest = out_ref.shape[0] - width - 1
    out_ref[width + 1 :] = jnp.zeros((rest, target.shape[1]), F32)


def query_grad_into(g_refs, sg_refs, target):
    put_split(g_refs, dot3(*split(target), *both(sg_refs), NN))


def source_into(x_out, state_out, square_ref, g_refs, source, state):
    width = source.shape[0]
    gradient = dot3(*split(square_ref[:width]), *both(g_refs), NN)
    x_out[...], state_out[...] = adagrad(source, state, gradient)


def pack_into(out_ref, parts, kinds):
    width = parts[0][1].shape[0]
    full, tail = divmod(width, LANES)
    span = tail_span(width, kinds)
    packed_tail = None
    for kind in range(kinds):
        total = sum(jnp.where(index == kind, part, 0.0) for index, part in parts)
        for block in range(full):
            start = (kind * full + block) * width
            out_ref[start : start + width] = total[:, block * LANES : (block + 1) * LANES]
        if tail:
            ends = pad_rows(total[:, full * LANES :], round_up(width, span))
            for place in range(ends.shape[0] // span):
                turn = (kind * (ends.shape[0] // span) + place) * tail
                moved = ends[place * span : (place + 1) * span]
                moved = pltpu.roll(moved, turn, 1) if turn else moved
                packed_tail = moved if packed_tail is None else packed_tail + moved
    start = kinds * full * width
    if tail:
        out_ref[start : start + span] = packed_tail
        start += span
    out_ref[start:] = jnp.zeros((out_ref.shape[0] - start, LANES), F32)


def tail_span(width, kinds):
    tail = width % LANES
    return round_up(-(-width // (LANES // tail // kinds)), 8) if tail else 0


def packed_rows(width, kinds, pieces):
    return round_up(kinds * (width // LANES) * width + tail_span(width, kinds), 8 * pieces)


def unpack(flat_ref, scaled_out, kinds, width, scale):
    full, tail = divmod(width, LANES)
    span = tail_span(width, kinds)
    for kind in range(kinds):
        for block in range(full):
            start = (kind * full + block) * width
            scaled_out[kind, :, block * LANES : (block + 1) * LANES] = scale * flat_ref[start : start + width]
        if tail:
            start = kinds * full * width
            ends = flat_ref[start : start + span]
            places = -(-width // span)
            for place in range(places):
                rows = min(span, width - place * span)
                turn = (kind * places + place) * tail
                moved = pltpu.roll(ends, LANES - turn, 1) if turn else ends
                scaled_out[kind, place * span : place * span + rows, full * LANES :] = scale * moved[:rows, :tail]


def put_pieces(out_ref, in_ref, me, pieces):
    rows = in_ref.shape[0] // pieces
    for piece in range(pieces):
        out_ref[piece * rows : (piece + 1) * rows] = in_ref[pl.ds(pl.multiple_of((me ^ piece) * rows, 8), rows)]


def first_kernel(ids, me, partners, relations, source, target, *refs, bucket, updated):
    if updated:
        target_out, sgh, sgl, square, xh, xl, qh, ql = refs
        square_of(square, relations[ids[bucket]])
        put_split((xh, xl), source[...])
        body, state = target[: source.shape[0]], target[source.shape[0] : source.shape[0] + 1]
        queries_into((qh, ql), square, (xh, xl), source.shape[0])
    else:
        target_state, target_out, sgh, sgl, square, xh, xl, qh, ql, matrix, source_in, target_in, sems = refs
        loads = [
            pltpu.make_async_copy(relations.at[ids[bucket]], matrix, sems.at[0]),
            pltpu.make_async_copy(source, source_in, sems.at[1]),
            pltpu.make_async_copy(target, target_in, sems.at[2]),
        ]
        for load in loads:
            load.start()
        loads[0].wait()
        square_of(square, matrix[...])
        loads[1].wait()
        put_split((xh, xl), source_in[...])
        queries_into((qh, ql), square, (xh, xl), source.shape[0])
        loads[2].wait()
        body, state = target_in[...], target_state[0]
    score_grad_into((sgh, sgl), (qh, ql), body, partners[bucket, 0])
    target_into(target_out, (qh, ql), (sgh, sgl), body, state)


def update_kernel(me, packed, relations, *refs, pieces, scale, place, last):
    grads_out, relations_out, flat, scaled, sems = refs[1 if place else 0 :][:5]
    kinds, width = relations.shape[0], relations.shape[1]
    put_pieces(flat, packed, me[0], pieces)
    unpack(flat, scaled, kinds, width, scale)
    stores = [pltpu.make_async_copy(scaled, grads_out.at[place], sems.at[0])]
    stores[0].start()
    renewed = refs[-1] if last else relations_out
    for kind in range(kinds):
        renewed[kind] = relations[kind] - operator_rate * scaled[kind]
    if last:
        stores.append(pltpu.make_async_copy(renewed, relations_out, sems.at[1]))
        stores[1].start()
    for store in stores:
        store.wait()


def second_kernel(ids, relations, source, source_state, target, sgh, sgl, source_out, state_out, grad_out, qh, ql, square, xh, xl, gh, gl, *, bucket):
    width = source.shape[0]
    query_grad_into((gh, gl), (sgh, sgl), target[:width])
    put_split((xh, xl), source[...])
    grad_out[...] = dot3(*both((xh, xl), width), *both((gh, gl)), NT)
    square_of(square, relations[ids[bucket]])
    source_into(source_out, state_out.at[0], square, (gh, gl), source[...], source_state[0])
    square_of(square, relations[ids[bucket + 1]])
    put_split((xh, xl), source_out[...])
    queries_into((qh, ql), square, (xh, xl), width)


def third_kernel(ids, me, partners, source, target, qh, ql, grad_before, packed, sgh, sgl, gh, gl, flat, *, bucket, kinds, pieces):
    width = source.shape[0]
    body = target[:width]
    score_grad_into((sgh, sgl), (qh, ql), body, partners[bucket, 0])
    query_grad_into((gh, gl), (sgh, sgl), body)
    grad = dot3(*split(source[...]), *both((gh, gl)), NT)
    pack_into(flat, ((ids[bucket - 1], grad_before[...]), (ids[bucket], grad)), kinds)
    put_pieces(packed, flat, me[0], pieces)


def fourth_kernel(ids, relations, source, source_state, target, qh, ql, sgh, sgl, gh, gl, target_out, source_out, state_out, square, *, bucket):
    width = source.shape[0]
    target_into(target_out, (qh, ql), (sgh, sgl), target[:width], target[width : width + 1])
    square_of(square, relations[ids[bucket]])
    source_into(source_out, state_out.at[0], square, (gh, gl), source[...], source_state[0])


VMEM = pl.BlockSpec(memory_space=pltpu.VMEM)
SMEM = pl.BlockSpec(memory_space=pltpu.SMEM)
HBM = pl.BlockSpec(memory_space=pltpu.HBM)


def call(kernel, name, args, args_in, outs, scratch=(), flops=0, outs_in=None, aliases=None):
    return pl.pallas_call(
        kernel,
        in_specs=args_in,
        out_specs=outs_in or [VMEM] * len(outs),
        out_shape=[jax.ShapeDtypeStruct(shape, dtype) for shape, dtype in outs],
        scratch_shapes=[pltpu.VMEM(*s) if isinstance(s, tuple) else s for s in scratch],
        input_output_aliases=aliases or {},
        compiler_params=pltpu.CompilerParams(vmem_limit_bytes=VMEM_LIMIT),
        cost_estimate=pl.CostEstimate(flops=flops, transcendentals=0, bytes_accessed=0),
        name=name,
    )(*args)


VMEM_LIMIT = 16 << 20


def shards(source_rows, source_state, target_rows, destination_state, positives, relation_ids, relations):
    buckets, kinds, width = positives.shape[0], relations.shape[0], relations.shape[1]
    source, state = source_rows[0, 0], source_state
    target, target_state = target_rows[0, 0], destination_state
    columns, block = source.shape[1], target.shape[1]
    scale = grad_gain / math.sqrt(columns * lax.axis_size("blk") * lax.axis_size("grp"))
    pieces, me = piece_plan()
    me, ids = me[None], relation_ids[:, 0, 0]
    wide, tall = round_up(width, LANES), round_up(width + 1, 8)
    rows = packed_rows(width, kinds, pieces)
    q_pair = [((wide, columns), BF16)] * 2
    sg_pair = [((block, columns), BF16)] * 2
    square = [((wide, wide), F32)]
    moving = [((tall, block), F32)]
    source_outs = [((width, columns), F32), (source_state.shape, F32)]
    product = 6 * width * width * columns
    updates = buckets // 2
    grads = ()
    for update in range(updates):
        bucket = 2 * update
        args, args_in, extra = (ids, me, positives, relations, source, target), [SMEM] * 2 + [VMEM] * 4, []
        if update == 0:
            args, args_in = args + (target_state,), [SMEM] * 2 + [VMEM] + [HBM] * 3 + [VMEM]
            extra = [((width, width), F32), (source.shape, F32), (target.shape, F32), pltpu.SemaphoreType.DMA((3,))]
        after, sgh, sgl = call(
            functools.partial(first_kernel, bucket=bucket, updated=update > 0), "first",
            args, args_in, moving + sg_pair, square + q_pair + q_pair + extra, 3 * product)
        arriving = from_behind(after, "blk", 1)
        source, state, grad, qh, ql = call(
            functools.partial(second_kernel, bucket=bucket), "second",
            (ids, relations, source, state, target, sgh, sgl), [SMEM] + [VMEM] * 6,
            source_outs + [((width, wide), F32)] + q_pair, square + q_pair + q_pair, 4 * product)
        target = arriving
        packed, sgh, sgl, gh, gl = call(
            functools.partial(third_kernel, bucket=bucket + 1, kinds=kinds, pieces=pieces), "third",
            (ids, me, positives, source, target, qh, ql, grad), [SMEM] * 2 + [VMEM] * 6,
            [((rows, LANES), F32)] + sg_pair + q_pair, [((rows, LANES), F32)], 3 * product)
        total, target, source, state = sum_everywhere(
            packed,
            lambda *args: call(
                functools.partial(fourth_kernel, bucket=bucket + 1), "fourth",
                (ids, *args), [SMEM] + [VMEM] * len(args), moving + source_outs, square, 2 * product),
            (relations, source, state, target, qh, ql, sgh, sgl, gh, gl))
        last = update == updates - 1
        grads, relations = call(
            functools.partial(update_kernel, pieces=pieces, scale=scale, place=update, last=last), "update",
            (me, total, relations, *((grads,) if update else ())), [SMEM, VMEM, VMEM] + ([HBM] if update else []),
            [((updates, *relations.shape), F32), (relations.shape, F32)],
            [((rows, LANES), F32), (relations.shape, F32), pltpu.SemaphoreType.DMA((2,))] + ([(relations.shape, F32)] if last else []),
            product, [HBM, HBM if last else VMEM], {3: 0} if update else None)
    return (
        source[None, None],
        state,
        target[None, None, :width],
        target[None, width : width + 1],
        relations,
        grads,
    )


def solution(mesh):
    rows, columns = P("blk", "grp", None, None), P("blk", "grp", None)
    in_specs = (rows, columns, rows, columns, P(None, "blk", "grp", None), P(None, "blk", "grp"), P())
    out_specs = (rows, columns, rows, columns, P(), P())
    return jax.shard_map(shards, mesh=mesh, in_specs=in_specs, out_specs=out_specs, check_vma=False)
```

```python
import functools
import math

import jax
import jax.numpy as jnp
from jax import lax
from jax.experimental import pallas as pl
from jax.experimental.pallas import tpu as pltpu
from jax.sharding import PartitionSpec as P

entity_rate = 0.1
operator_rate = 0.01
grad_gain = 6.0
AXES = ("blk", "grp")
LANES = 128
PART = 256
F32, BF16 = jnp.float32, jnp.bfloat16


def round_up(value, step):
    return -(-value // step) * step


def from_behind(value, axis, steps):
    count = lax.axis_size(axis)
    pairs = [(source, (source + steps) % count) for source in range(count)]
    return lax.ppermute(value, axis, pairs)


def exchange(value, blk_mask, grp_mask):
    blk, grp = lax.axis_size("blk"), lax.axis_size("grp")
    pairs = [(b * grp + g, (b ^ blk_mask) * grp + (g ^ grp_mask)) for b in range(blk) for g in range(grp)]
    return lax.ppermute(value, AXES, pairs)


def group_masks(bits):
    masks = []
    for member in range(1, 1 << len(bits)):
        blk_mask = sum(m for i, (axis, m) in enumerate(bits) if axis == "blk" and member >> i & 1)
        grp_mask = sum(m for i, (axis, m) in enumerate(bits) if axis == "grp" and member >> i & 1)
        masks.append((member, blk_mask, grp_mask))
    return sorted(masks, key=lambda t: -bin(t[0]).count("1"))


def own_member(bits):
    member = jnp.int32(0)
    for i, (axis, m) in enumerate(bits):
        member = member + (((lax.axis_index(axis) // m) % 2) << i)
    return member


def reduce_plan(blk, grp):
    if blk & (blk - 1) or grp & (grp - 1):
        return None
    blk_bits = [("blk", 1 << i) for i in range(blk.bit_length() - 1)]
    grp_bits = [("grp", 1 << i) for i in range(grp.bit_length() - 1)]
    stages = [s for s in (blk_bits[:1], blk_bits[1:3], grp_bits[:1]) if s]
    return (stages, blk_bits[3:] + grp_bits[1:]) if len(stages) > 1 else None


def scatter_sum(value, bits):
    blocks = value.reshape((1 << len(bits), -1) + value.shape[1:])
    total = blocks[0]
    for block in [exchange(blocks[d], mb, mg) for d, mb, mg in group_masks(bits)]:
        total = total + block
    return total


def gather(value, bits):
    arrived = {d: exchange(value, mb, mg) for d, mb, mg in group_masks(bits)}
    arrived[0] = value
    return jnp.concatenate([arrived[d] for d in range(1 << len(bits))], axis=0)


def piece_plan():
    plan = reduce_plan(lax.axis_size("blk"), lax.axis_size("grp"))
    if plan is None:
        return 1, jnp.int32(0)
    count, me = 1, jnp.int32(0)
    for stage in plan[0]:
        count <<= len(stage)
        me = (me << len(stage)) + own_member(stage)
    return count, me


def sum_everywhere(packed, work, args, work_on_arrival):
    plan = reduce_plan(lax.axis_size("blk"), lax.axis_size("grp"))
    if plan is None:
        after, *rest = work(*args)
        arriving = from_behind(after, "blk", 1)
        return lax.psum(packed, AXES), arriving, *rest, *(work_on_arrival(arriving) if work_on_arrival else ())
    stages, singles = plan
    for place, stage in enumerate(stages):
        if place == 1:
            packed, args = lax.optimization_barrier((packed, args))
            after, *rest = work(*args)
        packed = scatter_sum(packed, stage)
        if place == 1:
            packed, after = lax.optimization_barrier((packed, after))
            arriving = from_behind(after, "blk", 1)
    for axis, mask in singles:
        packed = packed + exchange(packed, mask if axis == "blk" else 0, mask if axis == "grp" else 0)
    for place, stage in reversed(list(enumerate(stages))):
        if place == 1:
            packed, arriving = lax.optimization_barrier((packed, arriving))
            rest += work_on_arrival(arriving) if work_on_arrival else []
        packed = gather(packed, stage)
        if place == 1:
            packed, rest = lax.optimization_barrier((packed, rest))
    return packed, arriving, *rest


NN = (((1,), (0,)), ((), ()))
NT = (((1,), (1,)), ((), ()))


def dot3(ah, al, bh, bl, dims):
    one = functools.partial(lax.dot_general, dimension_numbers=dims, preferred_element_type=F32)
    return one(ah, bh) + (one(ah, bl) + one(al, bh))


def split(x):
    high = x.astype(BF16)
    return high, (x - high.astype(F32)).astype(BF16)


def put_split(refs, x):
    rows = x.shape[0]
    refs[0][:rows], refs[1][:rows] = split(x)
    if rows < refs[0].shape[0]:
        blank = jnp.zeros((refs[0].shape[0] - rows, x.shape[1]), BF16)
        refs[0][rows:], refs[1][rows:] = blank, blank


def both(refs, rows=None):
    return (refs[0][...], refs[1][...]) if rows is None else (refs[0][:rows], refs[1][:rows])


def pad_rows(x, rows):
    return jnp.concatenate([x, jnp.zeros((rows - x.shape[0], x.shape[1]), x.dtype)], axis=0)


def square_of(pad_ref, matrix):
    width = matrix.shape[0]
    pad_ref[...] = jnp.zeros(pad_ref.shape, F32)
    pad_ref[:width, :width] = matrix


def parts_of(size):
    return [slice(start, min(start + PART, size)) for start in range(0, size, PART)]


def columns_of(refs, part, rows=None):
    return (refs[0][:rows, part], refs[1][:rows, part])


def split_columns(refs, compute):
    for part in parts_of(refs[0].shape[1]):
        high, low = split(compute(part))
        rows = high.shape[0]
        refs[0][:rows, part], refs[1][:rows, part] = high, low
        if rows < refs[0].shape[0]:
            blank = jnp.zeros((refs[0].shape[0] - rows, high.shape[1]), BF16)
            refs[0][rows:, part], refs[1][rows:, part] = blank, blank


def queries_into(q_refs, square_ref, x_refs, width):
    turned = split(square_ref[...].T[:width])
    split_columns(q_refs, lambda part: dot3(*turned, *columns_of(x_refs, part), NN))


def score_grad_into(sg_refs, scores, q_refs, target_turned, partner):
    for part in parts_of(scores.shape[1]):
        scores[:, part] = dot3(*target_turned, *columns_of(q_refs, part), NN)

    def gradient(part):
        score = scores[:, part]
        expo = jnp.exp(score - jnp.max(score, axis=0, keepdims=True))
        chance = expo * (1.0 / jnp.sum(expo, axis=0, keepdims=True))
        row = lax.broadcasted_iota(jnp.int32, score.shape, 0)
        return chance - jnp.where(row == partner[:, part], 1.0, 0.0)

    split_columns(sg_refs, gradient)


def adagrad(values, state, gradient):
    state_new = state + jnp.sum(gradient * gradient, axis=0, keepdims=True) * (1.0 / values.shape[0])
    return values - gradient * (entity_rate / jnp.sqrt(state_new)), state_new


def target_into(out_ref, q_refs, sg_refs, target, state):
    width = target.shape[0]
    for part in parts_of(target.shape[1]):
        gradient = dot3(*both(q_refs, width), sg_refs[0][part], sg_refs[1][part], NT)
        out_ref[:width, part], out_ref[width : width + 1, part] = adagrad(target[:, part], state[:, part], gradient)
    rest = out_ref.shape[0] - width - 1
    out_ref[width + 1 :] = jnp.zeros((rest, target.shape[1]), F32)


def query_grad_into(g_refs, sg_refs, target):
    halves = split(target)
    split_columns(g_refs, lambda part: dot3(*halves, *columns_of(sg_refs, part), NN))


def operator_grad(x_halves, g_refs):
    return jnp.concatenate(
        [dot3(*x_halves, g_refs[0][part], g_refs[1][part], NT) for part in parts_of(g_refs[0].shape[0])], axis=1)


def source_into(x_out, state_out, square_ref, g_refs, source, state):
    halves = split(square_ref[: source.shape[0]])
    for part in parts_of(source.shape[1]):
        gradient = dot3(*halves, *columns_of(g_refs, part), NN)
        x_out[:, part], state_out[:, part] = adagrad(source[:, part], state[:, part], gradient)


def pack_into(out_ref, parts, kinds):
    width = parts[0][1].shape[0]
    full, tail = divmod(width, LANES)
    span = tail_span(width, kinds)
    packed_tail = None
    for kind in range(kinds):
        total = sum(jnp.where(index == kind, part, 0.0) for index, part in parts)
        for block in range(full):
            start = (kind * full + block) * width
            out_ref[start : start + width] = total[:, block * LANES : (block + 1) * LANES]
        if tail:
            ends = pad_rows(total[:, full * LANES :], round_up(width, span))
            for place in range(ends.shape[0] // span):
                turn = (kind * (ends.shape[0] // span) + place) * tail
                moved = ends[place * span : (place + 1) * span]
                moved = pltpu.roll(moved, turn, 1) if turn else moved
                packed_tail = moved if packed_tail is None else packed_tail + moved
    start = kinds * full * width
    if tail:
        out_ref[start : start + span] = packed_tail
        start += span
    out_ref[start:] = jnp.zeros((out_ref.shape[0] - start, LANES), F32)


def tail_span(width, kinds):
    tail = width % LANES
    return round_up(-(-width // (LANES // tail // kinds)), 8) if tail else 0


def packed_rows(width, kinds, pieces):
    return round_up(kinds * (width // LANES) * width + tail_span(width, kinds), 8 * pieces)


def unpack(flat_ref, scaled_out, kind, width, scale):
    kinds, (full, tail) = scaled_out.shape[0], divmod(width, LANES)
    span = tail_span(width, kinds)
    for block in range(full):
        start = (kind * full + block) * width
        scaled_out[kind, :, block * LANES : (block + 1) * LANES] = scale * flat_ref[start : start + width]
    if tail:
        start = kinds * full * width
        ends = flat_ref[start : start + span]
        places = -(-width // span)
        for place in range(places):
            rows = min(span, width - place * span)
            turn = (kind * places + place) * tail
            moved = pltpu.roll(ends, LANES - turn, 1) if turn else ends
            scaled_out[kind, place * span : place * span + rows, full * LANES :] = scale * moved[:rows, :tail]


def put_pieces(out_ref, in_ref, me, pieces):
    rows = in_ref.shape[0] // pieces
    for piece in range(pieces):
        out_ref[piece * rows : (piece + 1) * rows] = in_ref[pl.ds(pl.multiple_of((me ^ piece) * rows, 8), rows)]


def opening_kernel(me, ids, partners, relations, source, target, target_state, target_out, sgh, sgl, square, xh, xl, qh, ql, scores, matrix, source_in, target_in, state_in, partners_in, ids_in, sems):
    width = source.shape[0]
    pairs = ((ids, ids_in), (source, source_in), (relations, matrix), (target, target_in), (target_state, state_in), (partners.at[0], partners_in))
    loads = [pltpu.make_async_copy(here, there, sems.at[place]) for place, (here, there) in enumerate(pairs)]
    for load in loads:
        load.start()
    loads[1].wait()
    put_split((xh, xl), source_in[...])
    loads[0].wait()
    loads[2].wait()
    square_of(square, matrix[ids_in[0]])
    queries_into((qh, ql), square, (xh, xl), width)
    for load in loads[3:]:
        load.wait()
    body = target_in[...]
    score_grad_into((sgh, sgl), scores, (qh, ql), split(pad_rows(body, qh.shape[0]).T), partners_in[0])
    target_into(target_out, (qh, ql), (sgh, sgl), body, state_in[0])


def prepare_kernel(target, yh, yl, *, width):
    yh[...], yl[...] = split(pad_rows(target[:width], yh.shape[1]).T)


def renew(flat, relations, scaled, renewed, kind, scale):
    unpack(flat, scaled, kind, relations.shape[1], scale)
    renewed[kind] = relations[kind] - operator_rate * scaled[kind]


def first_kernel(ids, me, partners, packed, relations, xh, xl, target, yh, yl, relations_out, scaled, target_out, sgh, sgl, flat, square, qh, ql, scores, *, bucket, pieces, scale):
    width = relations.shape[1]
    put_pieces(flat, packed, me[0], pieces)
    for kind in range(relations.shape[0]):
        renew(flat, relations, scaled, relations_out, kind, scale)
    square_of(square, relations_out[ids[bucket]])
    queries_into((qh, ql), square, (xh, xl), width)
    score_grad_into((sgh, sgl), scores, (qh, ql), both((yh, yl)), partners[bucket, 0])
    target_into(target_out, (qh, ql), (sgh, sgl), target[:width], target[width : width + 1])


def closing_kernel(me, packed, relations, *refs, pieces, scale, place):
    grads_out, relations_out, flat, scaled, renewed, sems = refs[1 if place else 0 :]
    put_pieces(flat, packed, me[0], pieces)
    stores = []
    for kind in range(relations.shape[0]):
        renew(flat, relations, scaled, renewed, kind, scale)
        for here, there in ((scaled, grads_out.at[place]), (renewed, relations_out)):
            stores.append(pltpu.make_async_copy(here.at[kind], there.at[kind], sems.at[len(stores)]))
            stores[-1].start()
    for store in stores:
        store.wait()


def second_kernel(ids, relations, source, source_state, target, sgh, sgl, *refs, bucket, place):
    if place is None:
        source_out, state_out, grad_out, qh, ql, xh, xl, square, gh, gl = refs
    else:
        scaled, *refs = refs
        source_out, state_out, grad_out, qh, ql, xh, xl, grads_out, square, gh, gl, sem = refs[1 if place else 0 :]
        store = pltpu.make_async_copy(scaled, grads_out.at[place], sem.at[0])
        store.start()
    width = source.shape[0]
    query_grad_into((gh, gl), (sgh, sgl), target[:width])
    put_split((xh, xl), source[...])
    grad_out[...] = operator_grad(both((xh, xl), width), (gh, gl))
    square_of(square, relations[ids[bucket]])
    source_into(source_out, state_out.at[0], square, (gh, gl), source[...], source_state[0])
    square_of(square, relations[ids[bucket + 1]])
    put_split((xh, xl), source_out[...])
    queries_into((qh, ql), square, (xh, xl), width)
    if place is not None:
        store.wait()


def third_kernel(ids, me, partners, xh, xl, target, qh, ql, grad_before, packed, sgh, sgl, gh, gl, flat, scores, *, bucket, kinds, pieces):
    width = grad_before.shape[0]
    body = target[:width]
    score_grad_into((sgh, sgl), scores, (qh, ql), split(pad_rows(body, qh.shape[0]).T), partners[bucket, 0])
    query_grad_into((gh, gl), (sgh, sgl), body)
    grad = operator_grad(both((xh, xl), width), (gh, gl))
    pack_into(flat, ((ids[bucket - 1], grad_before[...]), (ids[bucket], grad)), kinds)
    put_pieces(packed, flat, me[0], pieces)


def fourth_kernel(ids, relations, source, source_state, target, qh, ql, sgh, sgl, gh, gl, target_out, source_out, state_out, *refs, bucket):
    width = source.shape[0]
    target_into(target_out, (qh, ql), (sgh, sgl), target[:width], target[width : width + 1])
    square = refs[-1]
    square_of(square, relations[ids[bucket]])
    source_into(source_out, state_out.at[0], square, (gh, gl), source[...], source_state[0])
    if len(refs) > 1:
        put_split(refs[:2], source_out[...])


VMEM = pl.BlockSpec(memory_space=pltpu.VMEM)
SMEM = pl.BlockSpec(memory_space=pltpu.SMEM)
HBM = pl.BlockSpec(memory_space=pltpu.HBM)


def in_hbm(x):
    return pltpu.with_memory_space_constraint(x, pltpu.HBM)


def call(kernel, name, args, args_in, outs, scratch=(), flops=0, outs_in=None, aliases=None):
    return pl.pallas_call(
        kernel,
        in_specs=args_in,
        out_specs=outs_in or [VMEM] * len(outs),
        out_shape=[jax.ShapeDtypeStruct(shape, dtype) for shape, dtype in outs],
        scratch_shapes=[pltpu.VMEM(*s) if isinstance(s, tuple) else s for s in scratch],
        input_output_aliases=aliases or {},
        compiler_params=pltpu.CompilerParams(vmem_limit_bytes=VMEM_LIMIT),
        cost_estimate=pl.CostEstimate(flops=flops, transcendentals=0, bytes_accessed=0),
        name=name,
    )(*args)


VMEM_LIMIT = 16 << 20


def shards(source_rows, source_state, target_rows, destination_state, positives, relation_ids, relations):
    buckets, kinds, width = positives.shape[0], relations.shape[0], relations.shape[1]
    source, state = source_rows[0, 0], source_state
    target, target_state = target_rows[0, 0], destination_state
    columns, block = source.shape[1], target.shape[1]
    scale = grad_gain / math.sqrt(columns * lax.axis_size("blk") * lax.axis_size("grp"))
    pieces, me = piece_plan()
    me, ids = me[None], relation_ids[:, 0, 0]
    wide, tall = round_up(width, LANES), round_up(width + 1, 8)
    rows = packed_rows(width, kinds, pieces)
    q_pair = [((wide, columns), BF16)] * 2
    sg_pair = [((block, columns), BF16)] * 2
    square = [((wide, wide), F32)]
    moving = [((tall, block), F32)]
    scores = [((block, columns), F32)]
    source_outs = [((width, columns), F32), (source_state.shape, F32)]
    product = 6 * width * width * columns
    updates = buckets // 2
    rel_out, flat, y_pair = (relations.shape, F32), ((rows, LANES), F32), [((block, wide), BF16)] * 2
    grads, grads_out = None, ((updates, *relations.shape), F32)
    for update in range(updates):
        bucket, last = 2 * update, update == updates - 1
        if update == 0:
            after, sgh, sgl = call(
                opening_kernel, "opening",
                [me, *(in_hbm(x) for x in (ids, positives, relations, source, target, target_state))], [SMEM] + [HBM] * 6, moving + sg_pair,
                square + q_pair + q_pair + scores + [
                    (relations.shape, F32), (source.shape, F32), (target.shape, F32), (target_state.shape, F32),
                    (positives.shape[1:], jnp.int32), pltpu.SMEM(ids.shape, jnp.int32), pltpu.SemaphoreType.DMA((6,))],
                3 * product)
        else:
            relations, scaled, after, sgh, sgl = call(
                functools.partial(first_kernel, bucket=bucket, pieces=pieces, scale=scale), "first",
                (ids, me, positives, total, relations, xh, xl, target, yh, yl), [SMEM] * 2 + [VMEM] * 8,
                [rel_out, rel_out] + moving + sg_pair, [flat] + square + q_pair + scores, 3 * product)
        arriving = from_behind(after, "blk", 1)
        args, outs = (ids, relations, source, state, target, sgh, sgl), source_outs + [((width, wide), F32)] + q_pair + q_pair
        if update == 0:
            source, state, grad, qh, ql, xh, xl = call(
                functools.partial(second_kernel, bucket=bucket, place=None), "second",
                args, [SMEM] + [VMEM] * 6, outs, square + q_pair, 4 * product)
        else:
            before = () if grads is None else (grads,)
            source, state, grad, qh, ql, xh, xl, grads = call(
                functools.partial(second_kernel, bucket=bucket, place=update - 1), "second",
                (*args, scaled, *before), [SMEM] + [VMEM] * 7 + [HBM] * len(before), outs + [grads_out],
                square + q_pair + [pltpu.SemaphoreType.DMA((1,))], 4 * product,
                [VMEM] * len(outs) + [HBM], {8: len(outs)} if before else None)
        target = arriving
        packed, sgh, sgl, gh, gl = call(
            functools.partial(third_kernel, bucket=bucket + 1, kinds=kinds, pieces=pieces), "third",
            (ids, me, positives, xh, xl, target, qh, ql, grad), [SMEM] * 2 + [VMEM] * 7,
            [flat] + sg_pair + q_pair, [flat] + scores, 3 * product)
        total, target, source, state, *prepared = sum_everywhere(
            packed,
            lambda *args: call(
                functools.partial(fourth_kernel, bucket=bucket + 1), "fourth",
                (ids, *args), [SMEM] + [VMEM] * len(args), moving + source_outs + ([] if last else q_pair), square, 2 * product),
            (relations, source, state, target, qh, ql, sgh, sgl, gh, gl),
            None if last else lambda target: call(
                functools.partial(prepare_kernel, width=width), "prepare", (target,), [VMEM], y_pair, (), product // 4))
        if not last:
            xh, xl, yh, yl = prepared
    before = () if grads is None else (grads,)
    grads, relations = call(
        functools.partial(closing_kernel, pieces=pieces, scale=scale, place=updates - 1), "closing",
        (me, total, relations, *before), [SMEM, VMEM, VMEM] + [HBM] * len(before),
        [grads_out, rel_out], [flat, rel_out, rel_out, pltpu.SemaphoreType.DMA((2 * kinds,))],
        product, [HBM, HBM], {3: 0} if before else None)
    return (
        source[None, None],
        state,
        target[None, None, :width],
        target[None, width : width + 1],
        relations,
        grads,
    )


def solution(mesh):
    rows, columns = P("blk", "grp", None, None), P("blk", "grp", None)
    in_specs = (rows, columns, rows, columns, P(None, "blk", "grp", None), P(None, "blk", "grp"), P())
    out_specs = (rows, columns, rows, columns, P(), P())
    return jax.shard_map(shards, mesh=mesh, in_specs=in_specs, out_specs=out_specs, check_vma=False)
```

```python
import functools
import math

import jax
import jax.numpy as jnp
from jax import lax
from jax.experimental import pallas as pl
from jax.experimental.pallas import tpu as pltpu
from jax.sharding import PartitionSpec as P

entity_rate = 0.1
operator_rate = 0.01
grad_gain = 6.0
AXES = ("blk", "grp")
LANES = 128
PART = 256
F32, BF16 = jnp.float32, jnp.bfloat16


def round_up(value, step):
    return -(-value // step) * step


def from_behind(value, axis, steps):
    count = lax.axis_size(axis)
    pairs = [(source, (source + steps) % count) for source in range(count)]
    return lax.ppermute(value, axis, pairs)


def exchange(value, blk_mask, grp_mask):
    blk, grp = lax.axis_size("blk"), lax.axis_size("grp")
    pairs = [(b * grp + g, (b ^ blk_mask) * grp + (g ^ grp_mask)) for b in range(blk) for g in range(grp)]
    return lax.ppermute(value, AXES, pairs)


def group_masks(bits):
    masks = []
    for member in range(1, 1 << len(bits)):
        blk_mask = sum(m for i, (axis, m) in enumerate(bits) if axis == "blk" and member >> i & 1)
        grp_mask = sum(m for i, (axis, m) in enumerate(bits) if axis == "grp" and member >> i & 1)
        masks.append((member, blk_mask, grp_mask))
    return sorted(masks, key=lambda t: -bin(t[0]).count("1"))


def own_member(bits):
    member = jnp.int32(0)
    for i, (axis, m) in enumerate(bits):
        member = member + (((lax.axis_index(axis) // m) % 2) << i)
    return member


def reduce_plan(blk, grp):
    if blk & (blk - 1) or grp & (grp - 1):
        return None
    blk_bits = [("blk", 1 << i) for i in range(blk.bit_length() - 1)]
    grp_bits = [("grp", 1 << i) for i in range(grp.bit_length() - 1)]
    stages = [s for s in (blk_bits[:1], blk_bits[1:3], grp_bits[:2]) if s]
    return (stages, blk_bits[3:] + grp_bits[2:]) if len(stages) > 1 else None


def scatter_sum(value, bits):
    blocks = value.reshape((1 << len(bits), -1) + value.shape[1:])
    total = blocks[0]
    for block in [exchange(blocks[d], mb, mg) for d, mb, mg in group_masks(bits)]:
        total = total + block
    return total


def gather(value, bits):
    arrived = {d: exchange(value, mb, mg) for d, mb, mg in group_masks(bits)}
    arrived[0] = value
    return jnp.concatenate([arrived[d] for d in range(len(arrived))], axis=0)


def piece_plan():
    plan = reduce_plan(lax.axis_size("blk"), lax.axis_size("grp"))
    if plan is None:
        return 1, jnp.int32(0)
    count, me = 1, jnp.int32(0)
    for stage in plan[0]:
        count <<= len(stage)
        me = (me << len(stage)) + own_member(stage)
    return count, me


def sum_everywhere(packed, work, args, work_on_arrival):
    plan = reduce_plan(lax.axis_size("blk"), lax.axis_size("grp"))
    if plan is None:
        after, *rest = work(*args)
        arriving = from_behind(after, "blk", 1)
        return lax.psum(packed, AXES), arriving, *rest, *(work_on_arrival(arriving) if work_on_arrival else ())
    stages, singles = plan
    for place, stage in enumerate(stages):
        if place == 1:
            packed, args = lax.optimization_barrier((packed, args))
            after, *rest = work(*args)
        packed = scatter_sum(packed, stage)
        if place == 1:
            packed, after = lax.optimization_barrier((packed, after))
            arriving = from_behind(after, "blk", 1)
    for axis, mask in singles:
        packed = packed + exchange(packed, mask if axis == "blk" else 0, mask if axis == "grp" else 0)
    for place, stage in reversed(list(enumerate(stages))):
        if place == 1:
            packed, arriving = lax.optimization_barrier((packed, arriving))
            rest += work_on_arrival(arriving) if work_on_arrival else []
        packed = gather(packed, stage)
        if place == 1:
            packed, rest = lax.optimization_barrier((packed, rest))
    return packed, arriving, *rest


NN = (((1,), (0,)), ((), ()))
NT = (((1,), (1,)), ((), ()))


def dot3(ah, al, bh, bl, dims):
    one = functools.partial(lax.dot_general, dimension_numbers=dims, preferred_element_type=F32)
    return one(ah, bh) + (one(ah, bl) + one(al, bh))


def split(x):
    high = x.astype(BF16)
    return high, (x - high.astype(F32)).astype(BF16)


def put_split(refs, x):
    rows = x.shape[0]
    refs[0][:rows], refs[1][:rows] = split(x)
    if rows < refs[0].shape[0]:
        blank = jnp.zeros((refs[0].shape[0] - rows, x.shape[1]), BF16)
        refs[0][rows:], refs[1][rows:] = blank, blank


def both(refs, rows=None):
    return (refs[0][...], refs[1][...]) if rows is None else (refs[0][:rows], refs[1][:rows])


def pad_rows(x, rows):
    return jnp.concatenate([x, jnp.zeros((rows - x.shape[0], x.shape[1]), x.dtype)], axis=0)


def square_of(pad_ref, matrix):
    width = matrix.shape[0]
    pad_ref[...] = jnp.zeros(pad_ref.shape, F32)
    pad_ref[:width, :width] = matrix


def parts_of(size):
    return [slice(start, min(start + PART, size)) for start in range(0, size, PART)]


def columns_of(refs, part, rows=None):
    return (refs[0][:rows, part], refs[1][:rows, part])


def split_columns(refs, compute):
    for part in parts_of(refs[0].shape[1]):
        high, low = split(compute(part))
        rows = high.shape[0]
        refs[0][:rows, part], refs[1][:rows, part] = high, low
        if rows < refs[0].shape[0]:
            blank = jnp.zeros((refs[0].shape[0] - rows, high.shape[1]), BF16)
            refs[0][rows:, part], refs[1][rows:, part] = blank, blank


def queries_into(q_refs, square_ref, x_refs, width):
    turned = split(square_ref[...].T[:width])
    split_columns(q_refs, lambda part: dot3(*turned, *columns_of(x_refs, part), NN))


def score_grad_into(sg_refs, scores, q_refs, target_turned, partner):
    for part in parts_of(scores.shape[1]):
        scores[:, part] = dot3(*target_turned, *columns_of(q_refs, part), NN)

    def gradient(part):
        score = scores[:, part]
        expo = jnp.exp(score - jnp.max(score, axis=0, keepdims=True))
        chance = expo * (1.0 / jnp.sum(expo, axis=0, keepdims=True))
        row = lax.broadcasted_iota(jnp.int32, score.shape, 0)
        return chance - jnp.where(row == partner[:, part], 1.0, 0.0)

    split_columns(sg_refs, gradient)


def adagrad(values, state, gradient):
    state_new = state + jnp.sum(gradient * gradient, axis=0, keepdims=True) * (1.0 / values.shape[0])
    return values - gradient * (entity_rate / jnp.sqrt(state_new)), state_new


def target_into(out_ref, q_refs, sg_refs, target, state):
    width = target.shape[0]
    for part in parts_of(target.shape[1]):
        gradient = dot3(*both(q_refs, width), sg_refs[0][part], sg_refs[1][part], NT)
        out_ref[:width, part], out_ref[width : width + 1, part] = adagrad(target[:, part], state[:, part], gradient)
    rest = out_ref.shape[0] - width - 1
    out_ref[width + 1 :] = jnp.zeros((rest, target.shape[1]), F32)


def query_grad_into(g_refs, sg_refs, target):
    halves = split(target)
    split_columns(g_refs, lambda part: dot3(*halves, *columns_of(sg_refs, part), NN))


def operator_grad(x_halves, g_refs):
    return jnp.concatenate(
        [dot3(*x_halves, g_refs[0][part], g_refs[1][part], NT) for part in parts_of(g_refs[0].shape[0])], axis=1)


def source_into(x_out, state_out, square_ref, g_refs, source, state):
    halves = split(square_ref[: source.shape[0]])
    for part in parts_of(source.shape[1]):
        gradient = dot3(*halves, *columns_of(g_refs, part), NN)
        x_out[:, part], state_out[:, part] = adagrad(source[:, part], state[:, part], gradient)


class Pieces:
    def __init__(self, ref, me, count):
        self.ref, self.me, self.rows = ref, me, ref.shape[0] // count

    def runs(self, start, stop):
        while start < stop:
            piece, place = divmod(start, self.rows)
            end = min(stop, (piece + 1) * self.rows)
            first = pl.multiple_of((self.me ^ piece) * self.rows + place, 8)
            yield start, end, pl.ds(first, end - start)
            start = end

    def put(self, start, value):
        for first, end, here in self.runs(start, start + value.shape[0]):
            self.ref[here] = value[first - start : end - start]

    def get(self, start, size):
        found = [self.ref[here] for _, _, here in self.runs(start, start + size)]
        return jnp.concatenate(found, axis=0) if len(found) > 1 else found[0]


def pack_into(packed, parts, kinds):
    width = parts[0][1].shape[0]
    full, tail = divmod(width, LANES)
    span = tail_span(width, kinds)
    packed_tail = None
    for kind in range(kinds):
        total = sum(jnp.where(index == kind, part, 0.0) for index, part in parts)
        for block in range(full):
            packed.put((kind * full + block) * width, total[:, block * LANES : (block + 1) * LANES])
        if tail:
            ends = pad_rows(total[:, full * LANES :], round_up(width, span))
            for place in range(ends.shape[0] // span):
                turn = (kind * (ends.shape[0] // span) + place) * tail
                moved = ends[place * span : (place + 1) * span]
                moved = pltpu.roll(moved, turn, 1) if turn else moved
                packed_tail = moved if packed_tail is None else packed_tail + moved
    start = kinds * full * width
    if tail:
        packed.put(start, packed_tail)
        start += span
    packed.put(start, jnp.zeros((packed.ref.shape[0] - start, LANES), F32))


def tail_span(width, kinds):
    tail = width % LANES
    return round_up(-(-width // (LANES // tail // kinds)), 8) if tail else 0


def packed_rows(width, kinds, pieces):
    return round_up(kinds * (width // LANES) * width + tail_span(width, kinds), 8 * pieces)


def unpack(packed, scaled_out, kind, width, scale):
    kinds, (full, tail) = scaled_out.shape[0], divmod(width, LANES)
    span = tail_span(width, kinds)
    for block in range(full):
        scaled_out[kind, :, block * LANES : (block + 1) * LANES] = scale * packed.get((kind * full + block) * width, width)
    if tail:
        ends = packed.get(kinds * full * width, span)
        places = -(-width // span)
        for place in range(places):
            rows = min(span, width - place * span)
            turn = (kind * places + place) * tail
            moved = pltpu.roll(ends, LANES - turn, 1) if turn else ends
            scaled_out[kind, place * span : place * span + rows, full * LANES :] = scale * moved[:rows, :tail]


def opening_kernel(me, ids, partners, relations, source, target, target_state, target_out, sgh, sgl, square, xh, xl, qh, ql, scores, matrix, source_in, target_in, state_in, partners_in, ids_in, sems):
    width = source.shape[0]
    pairs = ((ids, ids_in), (relations, matrix), (source, source_in), (target, target_in), (target_state, state_in), (partners.at[0], partners_in))
    loads = [pltpu.make_async_copy(here, there, sems.at[place]) for place, (here, there) in enumerate(pairs)]
    for load in loads:
        load.start()
    loads[0].wait()
    loads[1].wait()
    square_of(square, matrix[ids_in[0]])
    loads[2].wait()
    put_split((xh, xl), source_in[...])
    queries_into((qh, ql), square, (xh, xl), width)
    for load in loads[3:]:
        load.wait()
    body = target_in[...]
    score_grad_into((sgh, sgl), scores, (qh, ql), split(pad_rows(body, qh.shape[0]).T), partners_in[0])
    target_into(target_out, (qh, ql), (sgh, sgl), body, state_in[0])


def prepare_kernel(target, yh, yl, *, width):
    yh[...], yl[...] = split(pad_rows(target[:width], yh.shape[1]).T)


def renew(packed, relations, scaled, renewed, kind, scale):
    unpack(packed, scaled, kind, relations.shape[1], scale)
    renewed[kind] = relations[kind] - operator_rate * scaled[kind]


def first_kernel(ids, me, partners, packed, relations, xh, xl, target, yh, yl, relations_out, scaled, target_out, sgh, sgl, square, qh, ql, scores, *, bucket, pieces, scale):
    width = relations.shape[1]
    for kind in range(relations.shape[0]):
        renew(Pieces(packed, me[0], pieces), relations, scaled, relations_out, kind, scale)
    square_of(square, relations_out[ids[bucket]])
    queries_into((qh, ql), square, (xh, xl), width)
    score_grad_into((sgh, sgl), scores, (qh, ql), both((yh, yl)), partners[bucket, 0])
    target_into(target_out, (qh, ql), (sgh, sgl), target[:width], target[width : width + 1])


def closing_kernel(me, packed, relations, *refs, pieces, scale, place):
    grads_out, relations_out, scaled, renewed, sems = refs[1 if place else 0 :]
    stores = []
    for kind in range(relations.shape[0]):
        renew(Pieces(packed, me[0], pieces), relations, scaled, renewed, kind, scale)
        for here, there in ((scaled, grads_out.at[place]), (renewed, relations_out)):
            stores.append(pltpu.make_async_copy(here.at[kind], there.at[kind], sems.at[len(stores)]))
            stores[-1].start()
    for store in stores:
        store.wait()


def second_kernel(ids, relations, source, source_state, target, sgh, sgl, *refs, bucket, place):
    if place is None:
        source_out, state_out, grad_out, qh, ql, xh, xl, square, gh, gl = refs
    else:
        scaled, *refs = refs
        source_out, state_out, grad_out, qh, ql, xh, xl, grads_out, square, gh, gl, sem = refs[1 if place else 0 :]
        store = pltpu.make_async_copy(scaled, grads_out.at[place], sem.at[0])
        store.start()
    width = source.shape[0]
    query_grad_into((gh, gl), (sgh, sgl), target[:width])
    put_split((xh, xl), source[...])
    grad_out[...] = operator_grad(both((xh, xl), width), (gh, gl))
    square_of(square, relations[ids[bucket]])
    source_into(source_out, state_out.at[0], square, (gh, gl), source[...], source_state[0])
    square_of(square, relations[ids[bucket + 1]])
    put_split((xh, xl), source_out[...])
    queries_into((qh, ql), square, (xh, xl), width)
    if place is not None:
        store.wait()


def third_kernel(ids, me, partners, xh, xl, target, qh, ql, grad_before, packed, sgh, sgl, gh, gl, scores, *, bucket, kinds, pieces):
    width = grad_before.shape[0]
    body = target[:width]
    score_grad_into((sgh, sgl), scores, (qh, ql), split(pad_rows(body, qh.shape[0]).T), partners[bucket, 0])
    query_grad_into((gh, gl), (sgh, sgl), body)
    grad = operator_grad(both((xh, xl), width), (gh, gl))
    pack_into(Pieces(packed, me[0], pieces), ((ids[bucket - 1], grad_before[...]), (ids[bucket], grad)), kinds)


def fourth_kernel(ids, relations, source, source_state, target, qh, ql, sgh, sgl, gh, gl, target_out, source_out, state_out, *refs, bucket):
    width = source.shape[0]
    target_into(target_out, (qh, ql), (sgh, sgl), target[:width], target[width : width + 1])
    square = refs[-1]
    square_of(square, relations[ids[bucket]])
    source_into(source_out, state_out.at[0], square, (gh, gl), source[...], source_state[0])
    if len(refs) > 1:
        put_split(refs[:2], source_out[...])


VMEM = pl.BlockSpec(memory_space=pltpu.VMEM)
SMEM = pl.BlockSpec(memory_space=pltpu.SMEM)
HBM = pl.BlockSpec(memory_space=pltpu.HBM)


def in_hbm(x):
    return pltpu.with_memory_space_constraint(x, pltpu.HBM)


def call(kernel, name, args, args_in, outs, scratch=(), flops=0, outs_in=None, aliases=None):
    return pl.pallas_call(
        kernel,
        in_specs=args_in,
        out_specs=outs_in or [VMEM] * len(outs),
        out_shape=[jax.ShapeDtypeStruct(shape, dtype) for shape, dtype in outs],
        scratch_shapes=[pltpu.VMEM(*s) if isinstance(s, tuple) else s for s in scratch],
        input_output_aliases=aliases or {},
        compiler_params=pltpu.CompilerParams(vmem_limit_bytes=VMEM_LIMIT),
        cost_estimate=pl.CostEstimate(flops=flops, transcendentals=0, bytes_accessed=0),
        name=name,
    )(*args)


VMEM_LIMIT = 16 << 20


def shards(source_rows, source_state, target_rows, destination_state, positives, relation_ids, relations):
    buckets, kinds, width = positives.shape[0], relations.shape[0], relations.shape[1]
    source, state = source_rows[0, 0], source_state
    target, target_state = target_rows[0, 0], destination_state
    columns, block = source.shape[1], target.shape[1]
    scale = grad_gain / math.sqrt(columns * lax.axis_size("blk") * lax.axis_size("grp"))
    pieces, me = piece_plan()
    me, ids = me[None], relation_ids[:, 0, 0]
    wide, tall = round_up(width, LANES), round_up(width + 1, 8)
    rows = packed_rows(width, kinds, pieces)
    q_pair = [((wide, columns), BF16)] * 2
    sg_pair = [((block, columns), BF16)] * 2
    square = [((wide, wide), F32)]
    moving = [((tall, block), F32)]
    scores = [((block, columns), F32)]
    source_outs = [((width, columns), F32), (source_state.shape, F32)]
    product = 6 * width * width * columns
    updates = buckets // 2
    rel_out, packed_out, y_pair = (relations.shape, F32), ((rows, LANES), F32), [((block, wide), BF16)] * 2
    grads, grads_out = None, ((updates, *relations.shape), F32)
    for update in range(updates):
        bucket, last = 2 * update, update == updates - 1
        if update == 0:
            after, sgh, sgl = call(
                opening_kernel, "opening",
                [me, *(in_hbm(x) for x in (ids, positives, relations, source, target, target_state))], [SMEM] + [HBM] * 6, moving + sg_pair,
                square + q_pair + q_pair + scores + [
                    (relations.shape, F32), (source.shape, F32), (target.shape, F32), (target_state.shape, F32),
                    (positives.shape[1:], jnp.int32), pltpu.SMEM(ids.shape, jnp.int32), pltpu.SemaphoreType.DMA((6,))],
                3 * product)
        else:
            relations, scaled, after, sgh, sgl = call(
                functools.partial(first_kernel, bucket=bucket, pieces=pieces, scale=scale), "first",
                (ids, me, positives, total, relations, xh, xl, target, yh, yl), [SMEM] * 2 + [VMEM] * 8,
                [rel_out, rel_out] + moving + sg_pair, square + q_pair + scores, 3 * product)
        arriving = from_behind(after, "blk", 1)
        args, outs = (ids, relations, source, state, target, sgh, sgl), source_outs + [((width, wide), F32)] + q_pair + q_pair
        if update == 0:
            source, state, grad, qh, ql, xh, xl = call(
                functools.partial(second_kernel, bucket=bucket, place=None), "second",
                args, [SMEM] + [VMEM] * 6, outs, square + q_pair, 4 * product)
        else:
            before = () if grads is None else (grads,)
            source, state, grad, qh, ql, xh, xl, grads = call(
                functools.partial(second_kernel, bucket=bucket, place=update - 1), "second",
                (*args, scaled, *before), [SMEM] + [VMEM] * 7 + [HBM] * len(before), outs + [grads_out],
                square + q_pair + [pltpu.SemaphoreType.DMA((1,))], 4 * product,
                [VMEM] * len(outs) + [HBM], {8: len(outs)} if before else None)
        target = arriving
        packed, sgh, sgl, gh, gl = call(
            functools.partial(third_kernel, bucket=bucket + 1, kinds=kinds, pieces=pieces), "third",
            (ids, me, positives, xh, xl, target, qh, ql, grad), [SMEM] * 2 + [VMEM] * 7,
            [packed_out] + sg_pair + q_pair, scores, 3 * product)
        total, target, source, state, *prepared = sum_everywhere(
            packed,
            lambda *args: call(
                functools.partial(fourth_kernel, bucket=bucket + 1), "fourth",
                (ids, *args), [SMEM] + [VMEM] * len(args), moving + source_outs + ([] if last else q_pair), square, 2 * product),
            (relations, source, state, target, qh, ql, sgh, sgl, gh, gl),
            None if last else lambda target: call(
                functools.partial(prepare_kernel, width=width), "prepare", (target,), [VMEM], y_pair, (), product // 4))
        if not last:
            xh, xl, yh, yl = prepared
    before = () if grads is None else (grads,)
    grads, relations = call(
        functools.partial(closing_kernel, pieces=pieces, scale=scale, place=updates - 1), "closing",
        (me, total, relations, *before), [SMEM, VMEM, VMEM] + [HBM] * len(before),
        [grads_out, rel_out], [rel_out, rel_out, pltpu.SemaphoreType.DMA((2 * kinds,))],
        product, [HBM, HBM], {3: 0} if before else None)
    return (
        source[None, None],
        state,
        target[None, None, :width],
        target[None, width : width + 1],
        relations,
        grads,
    )


def solution(mesh):
    rows, columns = P("blk", "grp", None, None), P("blk", "grp", None)
    in_specs = (rows, columns, rows, columns, P(None, "blk", "grp", None), P(None, "blk", "grp"), P())
    out_specs = (rows, columns, rows, columns, P(), P())
    return jax.shard_map(shards, mesh=mesh, in_specs=in_specs, out_specs=out_specs, check_vma=False)
```

```python
import functools
import math

import jax
import jax.numpy as jnp
from jax import lax
from jax.experimental import pallas as pl
from jax.experimental.pallas import tpu as pltpu
from jax.sharding import PartitionSpec as P

entity_rate = 0.1
operator_rate = 0.01
grad_gain = 6.0
AXES = ("blk", "grp")
LANES = 128
PART = 256
F32, BF16 = jnp.float32, jnp.bfloat16


def round_up(value, step):
    return -(-value // step) * step


def from_behind(value, axis, steps):
    count = lax.axis_size(axis)
    pairs = [(source, (source + steps) % count) for source in range(count)]
    return lax.ppermute(value, axis, pairs)


def exchange(value, blk_mask, grp_mask):
    blk, grp = lax.axis_size("blk"), lax.axis_size("grp")
    pairs = [(b * grp + g, (b ^ blk_mask) * grp + (g ^ grp_mask)) for b in range(blk) for g in range(grp)]
    return lax.ppermute(value, AXES, pairs)


def group_masks(bits):
    masks = []
    for member in range(1, 1 << len(bits)):
        blk_mask = sum(m for i, (axis, m) in enumerate(bits) if axis == "blk" and member >> i & 1)
        grp_mask = sum(m for i, (axis, m) in enumerate(bits) if axis == "grp" and member >> i & 1)
        masks.append((member, blk_mask, grp_mask))
    return sorted(masks, key=lambda t: -bin(t[0]).count("1"))


def own_member(bits):
    member = jnp.int32(0)
    for i, (axis, m) in enumerate(bits):
        member = member + (((lax.axis_index(axis) // m) % 2) << i)
    return member


def reduce_plan(blk, grp):
    if blk & (blk - 1) or grp & (grp - 1):
        return None
    blk_bits = [("blk", 1 << i) for i in range(blk.bit_length() - 1)]
    grp_bits = [("grp", 1 << i) for i in range(grp.bit_length() - 1)]
    stages = [s for s in (blk_bits[:1], blk_bits[1:3], grp_bits[:2]) if s]
    return (stages, blk_bits[3:] + grp_bits[2:]) if len(stages) > 1 else None


def scatter_sum(value, bits):
    blocks = value.reshape((1 << len(bits), -1) + value.shape[1:])
    total = blocks[0]
    for block in [exchange(blocks[d], mb, mg) for d, mb, mg in group_masks(bits)]:
        total = total + block
    return total


def gather(value, bits):
    arrived = {d: exchange(value, mb, mg) for d, mb, mg in group_masks(bits)}
    arrived[0] = value
    return jnp.concatenate([arrived[d] for d in range(len(arrived))], axis=0)


def piece_plan():
    plan = reduce_plan(lax.axis_size("blk"), lax.axis_size("grp"))
    if plan is None:
        return 1, jnp.int32(0)
    count, me = 1, jnp.int32(0)
    for stage in plan[0]:
        count <<= len(stage)
        me = (me << len(stage)) + own_member(stage)
    return count, me


def sum_everywhere(packed, work, args, work_on_arrival, work_on_half):
    plan = reduce_plan(lax.axis_size("blk"), lax.axis_size("grp"))
    if plan is None:
        after, *rest = work(*args)
        arriving = from_behind(after, "blk", 1)
        total = lax.psum(packed, AXES)
        middle = total.shape[0] // 2
        own, other = work_on_half(total[:middle]), total[middle:]
        return own, other, arriving, *rest, *work_on_arrival(arriving)
    stages, singles = plan
    for place, stage in enumerate(stages):
        if place == 1:
            packed, args = lax.optimization_barrier((packed, args))
            after, *rest = work(*args)
        packed = scatter_sum(packed, stage)
        if place == 1:
            packed, after = lax.optimization_barrier((packed, after))
            arriving = from_behind(after, "blk", 1)
    for axis, mask in singles:
        packed = packed + exchange(packed, mask if axis == "blk" else 0, mask if axis == "grp" else 0)
    for place, stage in reversed(list(enumerate(stages))[1:]):
        if place == 1:
            packed, arriving = lax.optimization_barrier((packed, arriving))
            rest += work_on_arrival(arriving)
        packed = gather(packed, stage)
        if place == 1:
            packed, rest = lax.optimization_barrier((packed, rest))
    other = exchange(packed, *group_masks(stages[0])[0][1:])
    return work_on_half(packed), other, arriving, *rest


NN = (((1,), (0,)), ((), ()))
NT = (((1,), (1,)), ((), ()))


def dot3(ah, al, bh, bl, dims):
    one = functools.partial(lax.dot_general, dimension_numbers=dims, preferred_element_type=F32)
    return one(ah, bh) + (one(ah, bl) + one(al, bh))


def split(x):
    high = x.astype(BF16)
    return high, (x - high.astype(F32)).astype(BF16)


def put_split(refs, x):
    rows = x.shape[0]
    refs[0][:rows], refs[1][:rows] = split(x)
    if rows < refs[0].shape[0]:
        blank = jnp.zeros((refs[0].shape[0] - rows, x.shape[1]), BF16)
        refs[0][rows:], refs[1][rows:] = blank, blank


def both(refs, rows=None):
    return (refs[0][...], refs[1][...]) if rows is None else (refs[0][:rows], refs[1][:rows])


def pad_rows(x, rows):
    return jnp.concatenate([x, jnp.zeros((rows - x.shape[0], x.shape[1]), x.dtype)], axis=0)


def square_of(pad_ref, matrix):
    width = matrix.shape[0]
    pad_ref[...] = jnp.zeros(pad_ref.shape, F32)
    pad_ref[:width, :width] = matrix


def parts_of(size):
    return [slice(start, min(start + PART, size)) for start in range(0, size, PART)]


def columns_of(refs, part, rows=None):
    return (refs[0][:rows, part], refs[1][:rows, part])


def split_columns(refs, compute):
    for part in parts_of(refs[0].shape[1]):
        high, low = split(compute(part))
        rows = high.shape[0]
        refs[0][:rows, part], refs[1][:rows, part] = high, low
        if rows < refs[0].shape[0]:
            blank = jnp.zeros((refs[0].shape[0] - rows, high.shape[1]), BF16)
            refs[0][rows:, part], refs[1][rows:, part] = blank, blank


def queries_into(q_refs, square_ref, x_refs, width):
    turned = split(square_ref[...].T[:width])
    split_columns(q_refs, lambda part: dot3(*turned, *columns_of(x_refs, part), NN))


def score_grad_into(sg_refs, scores, q_refs, target_turned, partner):
    for part in parts_of(scores.shape[1]):
        scores[:, part] = dot3(*target_turned, *columns_of(q_refs, part), NN)

    def gradient(part):
        score = scores[:, part]
        expo = jnp.exp(score - jnp.max(score, axis=0, keepdims=True))
        chance = expo * (1.0 / jnp.sum(expo, axis=0, keepdims=True))
        row = lax.broadcasted_iota(jnp.int32, score.shape, 0)
        return chance - jnp.where(row == partner[:, part], 1.0, 0.0)

    split_columns(sg_refs, gradient)


def adagrad(values, state, gradient):
    state_new = state + jnp.sum(gradient * gradient, axis=0, keepdims=True) * (1.0 / values.shape[0])
    return values - gradient * (entity_rate / jnp.sqrt(state_new)), state_new


def target_into(out_ref, q_refs, sg_refs, target, state):
    width = target.shape[0]
    for part in parts_of(target.shape[1]):
        gradient = dot3(*both(q_refs, width), sg_refs[0][part], sg_refs[1][part], NT)
        out_ref[:width, part], out_ref[width : width + 1, part] = adagrad(target[:, part], state[:, part], gradient)
    rest = out_ref.shape[0] - width - 1
    out_ref[width + 1 :] = jnp.zeros((rest, target.shape[1]), F32)


def query_grad_into(g_refs, sg_refs, target):
    halves = split(target)
    split_columns(g_refs, lambda part: dot3(*halves, *columns_of(sg_refs, part), NN))


def operator_grad(x_halves, g_refs):
    return jnp.concatenate(
        [dot3(*x_halves, g_refs[0][part], g_refs[1][part], NT) for part in parts_of(g_refs[0].shape[0])], axis=1)


def source_into(x_out, state_out, square_ref, g_refs, source, state):
    halves = split(square_ref[: source.shape[0]])
    for part in parts_of(source.shape[1]):
        gradient = dot3(*halves, *columns_of(g_refs, part), NN)
        x_out[:, part], state_out[:, part] = adagrad(source[:, part], state[:, part], gradient)


class Pieces:
    def __init__(self, ref, me, count):
        self.ref, self.me, self.rows = ref, me, ref.shape[0] // count

    def runs(self, start, stop):
        while start < stop:
            piece, place = divmod(start, self.rows)
            end = min(stop, (piece + 1) * self.rows)
            first = pl.multiple_of((self.me ^ piece) * self.rows + place, 8)
            yield start, end, pl.ds(first, end - start)
            start = end

    def put(self, start, value):
        for first, end, here in self.runs(start, start + value.shape[0]):
            self.ref[here] = value[first - start : end - start]

    def get(self, start, size):
        found = [self.ref[here] for _, _, here in self.runs(start, start + size)]
        return jnp.concatenate(found, axis=0) if len(found) > 1 else found[0]


def pack_into(packed, parts, kinds):
    width = parts[0][1].shape[0]
    full, tail = divmod(width, LANES)
    span, rows = tail_span(width), packed.ref.shape[0] // kinds
    for kind in range(kinds):
        total = sum(jnp.where(index == kind, part, 0.0) for index, part in parts)
        start = kind * rows
        for block in range(full):
            packed.put(start, total[:, block * LANES : (block + 1) * LANES])
            start += width
        if tail:
            ends, packed_tail = total[:, full * LANES :], None
            for place, first in enumerate(range(0, width, span)):
                moved = ends[first : first + span]
                moved = moved if moved.shape[0] == span else pad_rows(moved, span)
                moved = pltpu.roll(moved, place * tail, 1) if place else moved
                packed_tail = moved if packed_tail is None else packed_tail + moved
            packed.put(start, packed_tail)
            start += span
        if start < (kind + 1) * rows:
            packed.put(start, jnp.zeros(((kind + 1) * rows - start, LANES), F32))


def tail_span(width):
    tail = width % LANES
    return round_up(-(-width // (LANES // tail)), 8) if tail else 0


def packed_rows(width, kinds, pieces):
    return kinds * round_up((width // LANES) * width + tail_span(width), 8 * pieces)


def unpack(packed, place_of_kind, kinds, scaled_out, kind, scale):
    width, (full, tail) = scaled_out.shape[1], divmod(scaled_out.shape[1], LANES)
    start = place_of_kind * (packed.ref.shape[0] // kinds)
    for block in range(full):
        scaled_out[kind, :, block * LANES : (block + 1) * LANES] = scale * packed.get(start, width)
        start += width
    if tail:
        span = tail_span(width)
        ends = packed.get(start, span)
        for place, first in enumerate(range(0, width, span)):
            rows = min(span, width - first)
            moved = pltpu.roll(ends, LANES - place * tail, 1) if place else ends
            scaled_out[kind, first : first + rows, full * LANES :] = scale * moved[:rows, :tail]


def opening_kernel(me, ids, partners, relations, source, target, target_state, target_out, sgh, sgl, square, xh, xl, qh, ql, scores, matrix, source_in, target_in, state_in, partners_in, ids_in, sems):
    width = source.shape[0]
    pairs = ((ids, ids_in), (relations, matrix), (source, source_in), (target, target_in), (target_state, state_in), (partners.at[0], partners_in))
    loads = [pltpu.make_async_copy(here, there, sems.at[place]) for place, (here, there) in enumerate(pairs)]
    for load in loads:
        load.start()
    loads[0].wait()
    loads[1].wait()
    square_of(square, matrix[ids_in[0]])
    loads[2].wait()
    put_split((xh, xl), source_in[...])
    queries_into((qh, ql), square, (xh, xl), width)
    for load in loads[3:]:
        load.wait()
    body = target_in[...]
    score_grad_into((sgh, sgl), scores, (qh, ql), split(pad_rows(body, qh.shape[0]).T), partners_in[0])
    target_into(target_out, (qh, ql), (sgh, sgl), body, state_in[0])


def prepare_kernel(target, yh, yl, *, width):
    yh[...], yl[...] = split(pad_rows(target[:width], yh.shape[1]).T)


def renew(me, packed, relations, scaled, renewed, pieces, scale, half, done=None):
    kinds, count = relations.shape[0] // 2, max(pieces // 2, 1)
    for place in range(kinds):
        kind = ((me[0] // count) ^ half if pieces > 1 else half) * kinds + place
        unpack(Pieces(packed, me[0] % count, count), place, kinds, scaled, kind, scale)
        renewed[kind] = relations[kind] - operator_rate * scaled[kind]
        if done is not None:
            done(place, kind)


def own_kernel(me, packed, relations, scaled, renewed, *, pieces, scale):
    renew(me, packed, relations, scaled, renewed, pieces, scale, 0)


def first_kernel(ids, me, partners, packed, relations, own_scaled, own_renewed, xh, xl, target, yh, yl, scaled, renewed, target_out, sgh, sgl, square, qh, ql, scores, *, bucket, pieces, scale):
    width = relations.shape[1]
    renew(me, packed, relations, scaled, renewed, pieces, scale, 1)
    square_of(square, renewed[ids[bucket]])
    queries_into((qh, ql), square, (xh, xl), width)
    score_grad_into((sgh, sgl), scores, (qh, ql), both((yh, yl)), partners[bucket, 0])
    target_into(target_out, (qh, ql), (sgh, sgl), target[:width], target[width : width + 1])


def closing_kernel(me, packed, relations, *refs, pieces, scale, place, half):
    grads_out, relations_out, scaled, renewed, sems = refs[-5:]
    stores = []

    def store(slot, kind):
        for here, there in ((scaled, grads_out.at[place]), (renewed, relations_out)):
            stores.append(pltpu.make_async_copy(here.at[kind], there.at[kind], sems.at[len(stores)]))
            stores[-1].start()

    renew(me, packed, relations, scaled, renewed, pieces, scale, half, store)
    for copy in stores:
        copy.wait()


def second_kernel(ids, relations, source, source_state, target, sgh, sgl, *refs, bucket, place):
    if place is None:
        source_out, state_out, grad_out, qh, ql, xh, xl, square, gh, gl = refs
    else:
        scaled, *refs = refs
        source_out, state_out, grad_out, qh, ql, xh, xl, grads_out, square, gh, gl, sem = refs[1 if place else 0 :]
        store = pltpu.make_async_copy(scaled, grads_out.at[place], sem.at[0])
        store.start()
    width = source.shape[0]
    query_grad_into((gh, gl), (sgh, sgl), target[:width])
    put_split((xh, xl), source[...])
    grad_out[...] = operator_grad(both((xh, xl), width), (gh, gl))
    square_of(square, relations[ids[bucket]])
    source_into(source_out, state_out.at[0], square, (gh, gl), source[...], source_state[0])
    square_of(square, relations[ids[bucket + 1]])
    put_split((xh, xl), source_out[...])
    queries_into((qh, ql), square, (xh, xl), width)
    if place is not None:
        store.wait()


def third_kernel(ids, me, partners, xh, xl, target, qh, ql, grad_before, packed, sgh, sgl, gh, gl, scores, *, bucket, kinds, pieces):
    width = grad_before.shape[0]
    body = target[:width]
    score_grad_into((sgh, sgl), scores, (qh, ql), split(pad_rows(body, qh.shape[0]).T), partners[bucket, 0])
    query_grad_into((gh, gl), (sgh, sgl), body)
    grad = operator_grad(both((xh, xl), width), (gh, gl))
    pack_into(Pieces(packed, me[0], pieces), ((ids[bucket - 1], grad_before[...]), (ids[bucket], grad)), kinds)


def fourth_kernel(ids, relations, source, source_state, target, qh, ql, sgh, sgl, gh, gl, target_out, source_out, state_out, *refs, bucket):
    width = source.shape[0]
    target_into(target_out, (qh, ql), (sgh, sgl), target[:width], target[width : width + 1])
    square = refs[-1]
    square_of(square, relations[ids[bucket]])
    source_into(source_out, state_out.at[0], square, (gh, gl), source[...], source_state[0])
    if len(refs) > 1:
        put_split(refs[:2], source_out[...])


VMEM = pl.BlockSpec(memory_space=pltpu.VMEM)
SMEM = pl.BlockSpec(memory_space=pltpu.SMEM)
HBM = pl.BlockSpec(memory_space=pltpu.HBM)


def in_hbm(x):
    return pltpu.with_memory_space_constraint(x, pltpu.HBM)


def call(kernel, name, args, args_in, outs, scratch=(), flops=0, outs_in=None, aliases=None):
    return pl.pallas_call(
        kernel,
        in_specs=args_in,
        out_specs=outs_in or [VMEM] * len(outs),
        out_shape=[jax.ShapeDtypeStruct(shape, dtype) for shape, dtype in outs],
        scratch_shapes=[pltpu.VMEM(*s) if isinstance(s, tuple) else s for s in scratch],
        input_output_aliases=aliases or {},
        compiler_params=pltpu.CompilerParams(vmem_limit_bytes=VMEM_LIMIT),
        cost_estimate=pl.CostEstimate(flops=flops, transcendentals=0, bytes_accessed=0),
        name=name,
    )(*args)


VMEM_LIMIT = 16 << 20


def shards(source_rows, source_state, target_rows, destination_state, positives, relation_ids, relations):
    buckets, kinds, width = positives.shape[0], relations.shape[0], relations.shape[1]
    if kinds % 2 or buckets % 2 or width % 16:
        raise ValueError("unsupported shapes")
    source, state = source_rows[0, 0], source_state
    target, target_state = target_rows[0, 0], destination_state
    columns, block = source.shape[1], target.shape[1]
    scale = grad_gain / math.sqrt(columns * lax.axis_size("blk") * lax.axis_size("grp"))
    pieces, me = piece_plan()
    me, ids = me[None], relation_ids[:, 0, 0]
    wide, tall = round_up(width, LANES), round_up(width + 1, 8)
    rows = packed_rows(width, kinds, pieces)
    q_pair = [((wide, columns), BF16)] * 2
    sg_pair = [((block, columns), BF16)] * 2
    square = [((wide, wide), F32)]
    moving = [((tall, block), F32)]
    scores = [((block, columns), F32)]
    source_outs = [((width, columns), F32), (source_state.shape, F32)]
    product = 6 * width * width * columns
    updates = buckets // 2
    rel_out, packed_out, y_pair = (relations.shape, F32), ((rows, LANES), F32), [((block, wide), BF16)] * 2
    grads, grads_out = None, ((updates, *relations.shape), F32)
    for update in range(updates):
        bucket, last = 2 * update, update == updates - 1
        if update == 0:
            after, sgh, sgl = call(
                opening_kernel, "opening",
                [me, *(in_hbm(x) for x in (ids, positives, relations, source, target, target_state))], [SMEM] + [HBM] * 6, moving + sg_pair,
                square + q_pair + q_pair + scores + [
                    (relations.shape, F32), (source.shape, F32), (target.shape, F32), (target_state.shape, F32),
                    (positives.shape[1:], jnp.int32), pltpu.SMEM(ids.shape, jnp.int32), pltpu.SemaphoreType.DMA((6,))],
                3 * product)
        else:
            scaled, relations, after, sgh, sgl = call(
                functools.partial(first_kernel, bucket=bucket, pieces=pieces, scale=scale), "first",
                (ids, me, positives, other, relations, *own, xh, xl, target, yh, yl), [SMEM] * 2 + [VMEM] * 10,
                [rel_out, rel_out] + moving + sg_pair, square + q_pair + scores, 3 * product, aliases={5: 0, 6: 1})
        arriving = from_behind(after, "blk", 1)
        args, outs = (ids, relations, source, state, target, sgh, sgl), source_outs + [((width, wide), F32)] + q_pair + q_pair
        if update == 0:
            source, state, grad, qh, ql, xh, xl = call(
                functools.partial(second_kernel, bucket=bucket, place=None), "second",
                args, [SMEM] + [VMEM] * 6, outs, square + q_pair, 4 * product)
        else:
            before = () if grads is None else (grads,)
            source, state, grad, qh, ql, xh, xl, grads = call(
                functools.partial(second_kernel, bucket=bucket, place=update - 1), "second",
                (*args, scaled, *before), [SMEM] + [VMEM] * 7 + [HBM] * len(before), outs + [grads_out],
                square + q_pair + [pltpu.SemaphoreType.DMA((1,))], 4 * product,
                [VMEM] * len(outs) + [HBM], {8: len(outs)} if before else None)
        target = arriving
        packed, sgh, sgl, gh, gl = call(
            functools.partial(third_kernel, bucket=bucket + 1, kinds=kinds, pieces=pieces), "third",
            (ids, me, positives, xh, xl, target, qh, ql, grad), [SMEM] * 2 + [VMEM] * 7,
            [packed_out] + sg_pair + q_pair, scores, 3 * product)

        def close(half, own=None):
            before = tuple(own) if own is not None else () if grads is None else (grads,)
            return call(
                functools.partial(closing_kernel, pieces=pieces, scale=scale, place=updates - 1, half=0 if own is None else 1), "closing",
                (me, half, relations, *before), [SMEM, VMEM, VMEM] + [HBM] * len(before),
                [grads_out, rel_out], [rel_out, rel_out, pltpu.SemaphoreType.DMA((kinds,))],
                product // 4, [HBM, HBM], {3 + i: i for i in range(len(before))})

        own, other, target, source, state, *prepared = sum_everywhere(
            packed,
            lambda *args: call(
                functools.partial(fourth_kernel, bucket=bucket + 1), "fourth",
                (ids, *args), [SMEM] + [VMEM] * len(args), moving + source_outs + ([] if last else q_pair), square, 2 * product),
            (relations, source, state, target, qh, ql, sgh, sgl, gh, gl),
            (lambda target: [target[None, None, :width], target[None, width : width + 1]]) if last else lambda target: call(
                functools.partial(prepare_kernel, width=width), "prepare", (target,), [VMEM], y_pair, (), product // 4),
            close if last else lambda half: call(
                functools.partial(own_kernel, pieces=pieces, scale=scale), "own",
                (me, half, relations), [SMEM, VMEM, VMEM], [rel_out, rel_out], (), product // 4))
        if not last:
            xh, xl, yh, yl = prepared
    grads, relations = close(other, own)
    return (
        source[None, None],
        state,
        *prepared,
        relations,
        grads,
    )


def solution(mesh):
    rows, columns = P("blk", "grp", None, None), P("blk", "grp", None)
    in_specs = (rows, columns, rows, columns, P(None, "blk", "grp", None), P(None, "blk", "grp"), P())
    out_specs = (rows, columns, rows, columns, P(), P())
    return jax.shard_map(shards, mesh=mesh, in_specs=in_specs, out_specs=out_specs, check_vma=False)
```

```python
import functools
import math

import jax
import jax.numpy as jnp
from jax import lax
from jax.experimental import pallas as pl
from jax.experimental.pallas import tpu as pltpu
from jax.sharding import PartitionSpec as P

entity_rate = 0.1
operator_rate = 0.01
grad_gain = 6.0
AXES = ("blk", "grp")
LANES = 128
PART = 256
F32, BF16 = jnp.float32, jnp.bfloat16


def round_up(value, step):
    return -(-value // step) * step


def from_behind(value, axis, steps):
    count = lax.axis_size(axis)
    pairs = [(source, (source + steps) % count) for source in range(count)]
    return lax.ppermute(value, axis, pairs)


def exchange(value, blk_mask, grp_mask):
    blk, grp = lax.axis_size("blk"), lax.axis_size("grp")
    pairs = [(b * grp + g, (b ^ blk_mask) * grp + (g ^ grp_mask)) for b in range(blk) for g in range(grp)]
    return lax.ppermute(value, AXES, pairs)


def group_masks(bits):
    masks = []
    for member in range(1, 1 << len(bits)):
        blk_mask = sum(m for i, (axis, m) in enumerate(bits) if axis == "blk" and member >> i & 1)
        grp_mask = sum(m for i, (axis, m) in enumerate(bits) if axis == "grp" and member >> i & 1)
        masks.append((member, blk_mask, grp_mask))
    return sorted(masks, key=lambda t: -bin(t[0]).count("1"))


def own_member(bits):
    member = jnp.int32(0)
    for i, (axis, m) in enumerate(bits):
        member = member + (((lax.axis_index(axis) // m) % 2) << i)
    return member


def reduce_plan(blk, grp):
    if blk & (blk - 1) or grp & (grp - 1):
        return None
    blk_bits = [("blk", 1 << i) for i in range(blk.bit_length() - 1)]
    grp_bits = [("grp", 1 << i) for i in range(grp.bit_length() - 1)]
    stages = [s for s in (blk_bits[:1], blk_bits[1:3], grp_bits[:2]) if s]
    return (stages, blk_bits[3:] + grp_bits[2:]) if len(stages) > 1 else None


def scatter_sum(value, bits):
    blocks = value.reshape((1 << len(bits), -1) + value.shape[1:])
    total = blocks[0]
    for block in [exchange(blocks[d], mb, mg) for d, mb, mg in group_masks(bits)]:
        total = total + block
    return total


def gather(value, bits):
    arrived = {d: exchange(value, mb, mg) for d, mb, mg in group_masks(bits)}
    arrived[0] = value
    return jnp.concatenate([arrived[d] for d in range(len(arrived))], axis=0)


def piece_plan():
    plan = reduce_plan(lax.axis_size("blk"), lax.axis_size("grp"))
    if plan is None:
        return 1, jnp.int32(0)
    count, me = 1, jnp.int32(0)
    for stage in plan[0]:
        count <<= len(stage)
        me = (me << len(stage)) + own_member(stage)
    return count, me


def sum_everywhere(packed, work, args, work_on_arrival, work_on_half):
    plan = reduce_plan(lax.axis_size("blk"), lax.axis_size("grp"))
    if plan is None:
        after, *rest = work(*args)
        arriving = from_behind(after, "blk", 1)
        total = lax.psum(packed, AXES)
        middle = total.shape[0] // 2
        own, other = work_on_half(total[:middle]), total[middle:]
        return own, other, arriving, *rest, *work_on_arrival(arriving)
    stages, singles = plan
    for place, stage in enumerate(stages):
        if place == 1:
            packed, args = lax.optimization_barrier((packed, args))
            after, *rest = work(*args)
        packed = scatter_sum(packed, stage)
        if place == 1:
            packed, after = lax.optimization_barrier((packed, after))
            arriving = from_behind(after, "blk", 1)
    for axis, mask in singles:
        packed = packed + exchange(packed, mask if axis == "blk" else 0, mask if axis == "grp" else 0)
    for place, stage in reversed(list(enumerate(stages))[1:]):
        if place == 1:
            packed, arriving = lax.optimization_barrier((packed, arriving))
            rest += work_on_arrival(arriving)
        packed = gather(packed, stage)
        if place == 1:
            packed, rest = lax.optimization_barrier((packed, rest))
    other = exchange(packed, *group_masks(stages[0])[0][1:])
    return work_on_half(packed), other, arriving, *rest


NN = (((1,), (0,)), ((), ()))
NT = (((1,), (1,)), ((), ()))


def dot3(ah, al, bh, bl, dims):
    one = functools.partial(lax.dot_general, dimension_numbers=dims, preferred_element_type=F32)
    return one(ah, bh) + (one(ah, bl) + one(al, bh))


def split(x):
    high = x.astype(BF16)
    return high, (x - high.astype(F32)).astype(BF16)


def put_split(refs, x):
    rows = x.shape[0]
    refs[0][:rows], refs[1][:rows] = split(x)
    if rows < refs[0].shape[0]:
        blank = jnp.zeros((refs[0].shape[0] - rows, x.shape[1]), BF16)
        refs[0][rows:], refs[1][rows:] = blank, blank


def both(refs, rows=None):
    return (refs[0][...], refs[1][...]) if rows is None else (refs[0][:rows], refs[1][:rows])


def pad_rows(x, rows):
    return jnp.concatenate([x, jnp.zeros((rows - x.shape[0], x.shape[1]), x.dtype)], axis=0)


def square_of(pad_ref, matrix):
    width = matrix.shape[0]
    pad_ref[...] = jnp.zeros(pad_ref.shape, F32)
    pad_ref[:width, :width] = matrix


def parts_of(size):
    return [slice(start, min(start + PART, size)) for start in range(0, size, PART)]


def columns_of(refs, part, rows=None):
    return (refs[0][:rows, part], refs[1][:rows, part])


def split_columns(refs, compute):
    for part in parts_of(refs[0].shape[1]):
        high, low = split(compute(part))
        rows = high.shape[0]
        refs[0][:rows, part], refs[1][:rows, part] = high, low
        if rows < refs[0].shape[0]:
            blank = jnp.zeros((refs[0].shape[0] - rows, high.shape[1]), BF16)
            refs[0][rows:, part], refs[1][rows:, part] = blank, blank


def queries_into(q_refs, square_ref, x_refs, width):
    turned = split(square_ref[...].T[:width])
    split_columns(q_refs, lambda part: dot3(*turned, *columns_of(x_refs, part), NN))


def score_grad_into(sg_refs, scores, q_refs, target_turned, partner):
    for part in parts_of(scores.shape[1]):
        scores[:, part] = dot3(*target_turned, *columns_of(q_refs, part), NN)

    def gradient(part):
        score = scores[:, part]
        expo = jnp.exp(score - jnp.max(score, axis=0, keepdims=True))
        chance = expo * (1.0 / jnp.sum(expo, axis=0, keepdims=True))
        row = lax.broadcasted_iota(jnp.int32, score.shape, 0)
        return chance - jnp.where(row == partner[:, part], 1.0, 0.0)

    split_columns(sg_refs, gradient)


def adagrad(values, state, gradient):
    state_new = state + jnp.sum(gradient * gradient, axis=0, keepdims=True) * (1.0 / values.shape[0])
    return values - gradient * (entity_rate / jnp.sqrt(state_new)), state_new


def target_into(out_ref, q_refs, sg_refs, target, state):
    width = target.shape[0]
    for part in parts_of(target.shape[1]):
        gradient = dot3(*both(q_refs, width), sg_refs[0][part], sg_refs[1][part], NT)
        out_ref[:width, part], out_ref[width : width + 1, part] = adagrad(target[:, part], state[:, part], gradient)
    rest = out_ref.shape[0] - width - 1
    out_ref[width + 1 :] = jnp.zeros((rest, target.shape[1]), F32)


def query_grad_into(g_refs, sg_refs, target):
    halves = split(target)
    split_columns(g_refs, lambda part: dot3(*halves, *columns_of(sg_refs, part), NN))


def operator_grad(x_halves, g_refs):
    return jnp.concatenate(
        [dot3(*x_halves, g_refs[0][part], g_refs[1][part], NT) for part in parts_of(g_refs[0].shape[0])], axis=1)


def source_into(x_out, state_out, square_ref, g_refs, source, state):
    halves = split(square_ref[: source.shape[0]])
    for part in parts_of(source.shape[1]):
        gradient = dot3(*halves, *columns_of(g_refs, part), NN)
        x_out[:, part], state_out[:, part] = adagrad(source[:, part], state[:, part], gradient)


class Pieces:
    def __init__(self, ref, me, count):
        self.ref, self.me, self.rows = ref, me, ref.shape[0] // count

    def runs(self, start, stop):
        while start < stop:
            piece, place = divmod(start, self.rows)
            end = min(stop, (piece + 1) * self.rows)
            first = pl.multiple_of((self.me ^ piece) * self.rows + place, 8)
            yield start, end, pl.ds(first, end - start)
            start = end

    def put(self, start, value):
        for first, end, here in self.runs(start, start + value.shape[0]):
            self.ref[here] = value[first - start : end - start]

    def get(self, start, size):
        found = [self.ref[here] for _, _, here in self.runs(start, start + size)]
        return jnp.concatenate(found, axis=0) if len(found) > 1 else found[0]


def pack_into(packed, parts, kinds):
    width = parts[0][1].shape[0]
    full, tail = divmod(width, LANES)
    span, rows = tail_span(width), packed.ref.shape[0] // kinds
    for kind in range(kinds):
        total = sum(jnp.where(index == kind, part, 0.0) for index, part in parts)
        start = kind * rows
        for block in range(full):
            packed.put(start, total[:, block * LANES : (block + 1) * LANES])
            start += width
        if tail:
            ends, packed_tail = total[:, full * LANES :], None
            for place, first in enumerate(range(0, width, span)):
                moved = ends[first : first + span]
                moved = moved if moved.shape[0] == span else pad_rows(moved, span)
                moved = pltpu.roll(moved, place * tail, 1) if place else moved
                packed_tail = moved if packed_tail is None else packed_tail + moved
            packed.put(start, packed_tail)
            start += span
        if start < (kind + 1) * rows:
            packed.put(start, jnp.zeros(((kind + 1) * rows - start, LANES), F32))


def tail_span(width):
    tail = width % LANES
    return round_up(-(-width // (LANES // tail)), 8) if tail else 0


def packed_rows(width, kinds, pieces):
    return kinds * round_up((width // LANES) * width + tail_span(width), 8 * pieces)


def unpack(packed, place_of_kind, kinds, scaled_out, kind, scale):
    width, (full, tail) = scaled_out.shape[1], divmod(scaled_out.shape[1], LANES)
    start = place_of_kind * (packed.ref.shape[0] // kinds)
    for block in range(full):
        scaled_out[kind, :, block * LANES : (block + 1) * LANES] = scale * packed.get(start, width)
        start += width
    if tail:
        span = tail_span(width)
        ends = packed.get(start, span)
        for place, first in enumerate(range(0, width, span)):
            rows = min(span, width - first)
            moved = pltpu.roll(ends, LANES - place * tail, 1) if place else ends
            scaled_out[kind, first : first + rows, full * LANES :] = scale * moved[:rows, :tail]


def opening_kernel(me, ids, partners, relations, source, target, target_state, target_out, sgh, sgl, square, xh, xl, qh, ql, scores, matrix, source_in, target_in, state_in, partners_in, ids_in, sems):
    width = source.shape[0]
    pairs = ((ids, ids_in), (relations, matrix), (source, source_in), (target, target_in), (target_state, state_in), (partners.at[0], partners_in))
    loads = [pltpu.make_async_copy(here, there, sems.at[place]) for place, (here, there) in enumerate(pairs)]
    for load in loads:
        load.start()
    loads[0].wait()
    loads[1].wait()
    square_of(square, matrix[ids_in[0]])
    loads[2].wait()
    put_split((xh, xl), source_in[...])
    for load in loads[3:]:
        load.wait()
    body = target_in[...]
    turned = split(pad_rows(body, qh.shape[0]).T)
    queries_into((qh, ql), square, (xh, xl), width)
    score_grad_into((sgh, sgl), scores, (qh, ql), turned, partners_in[0])
    target_into(target_out, (qh, ql), (sgh, sgl), body, state_in[0])


def prepare_kernel(target, yh, yl, *, width):
    yh[...], yl[...] = split(pad_rows(target[:width], yh.shape[1]).T)


def renew(me, packed, relations, scaled, renewed, pieces, scale, half, done=None):
    kinds, count = relations.shape[0] // 2, max(pieces // 2, 1)
    for place in range(kinds):
        kind = ((me[0] // count) ^ half if pieces > 1 else half) * kinds + place
        unpack(Pieces(packed, me[0] % count, count), place, kinds, scaled, kind, scale)
        renewed[kind] = relations[kind] - operator_rate * scaled[kind]
        if done is not None:
            done(place, kind)


def own_kernel(me, packed, relations, scaled, renewed, *, pieces, scale):
    renew(me, packed, relations, scaled, renewed, pieces, scale, 0)


def first_kernel(ids, me, partners, packed, relations, own_scaled, own_renewed, xh, xl, target, yh, yl, scaled, renewed, target_out, sgh, sgl, square, qh, ql, scores, *, bucket, pieces, scale):
    width = relations.shape[1]
    renew(me, packed, relations, scaled, renewed, pieces, scale, 1)
    square_of(square, renewed[ids[bucket]])
    queries_into((qh, ql), square, (xh, xl), width)
    score_grad_into((sgh, sgl), scores, (qh, ql), both((yh, yl)), partners[bucket, 0])
    target_into(target_out, (qh, ql), (sgh, sgl), target[:width], target[width : width + 1])


def closing_kernel(me, packed, relations, *refs, pieces, scale, place, half):
    grads_out, relations_out, scaled, renewed, sems = refs[-5:]
    stores = []

    def store(slot, kind):
        for here, there in ((scaled, grads_out.at[place]), (renewed, relations_out)):
            stores.append(pltpu.make_async_copy(here.at[kind], there.at[kind], sems.at[len(stores)]))
            stores[-1].start()

    renew(me, packed, relations, scaled, renewed, pieces, scale, half, store)
    for copy in stores:
        copy.wait()


def second_kernel(ids, relations, source, source_state, target, sgh, sgl, *refs, bucket, place):
    if place is None:
        source_out, state_out, grad_out, qh, ql, xh, xl, square, gh, gl = refs
    else:
        scaled, *refs = refs
        source_out, state_out, grad_out, qh, ql, xh, xl, grads_out, square, gh, gl, sem = refs[1 if place else 0 :]
        store = pltpu.make_async_copy(scaled, grads_out.at[place], sem.at[0])
        store.start()
    width = source.shape[0]
    query_grad_into((gh, gl), (sgh, sgl), target[:width])
    put_split((xh, xl), source[...])
    grad_out[...] = operator_grad(both((xh, xl), width), (gh, gl))
    square_of(square, relations[ids[bucket]])
    source_into(source_out, state_out.at[0], square, (gh, gl), source[...], source_state[0])
    square_of(square, relations[ids[bucket + 1]])
    put_split((xh, xl), source_out[...])
    queries_into((qh, ql), square, (xh, xl), width)
    if place is not None:
        store.wait()


def third_kernel(ids, me, partners, xh, xl, target, qh, ql, grad_before, packed, sgh, sgl, gh, gl, scores, *, bucket, kinds, pieces):
    width = grad_before.shape[0]
    body = target[:width]
    score_grad_into((sgh, sgl), scores, (qh, ql), split(pad_rows(body, qh.shape[0]).T), partners[bucket, 0])
    query_grad_into((gh, gl), (sgh, sgl), body)
    grad = operator_grad(both((xh, xl), width), (gh, gl))
    pack_into(Pieces(packed, me[0], pieces), ((ids[bucket - 1], grad_before[...]), (ids[bucket], grad)), kinds)


def fourth_kernel(ids, relations, source, source_state, target, qh, ql, sgh, sgl, gh, gl, target_out, source_out, state_out, *refs, bucket):
    width = source.shape[0]
    target_into(target_out, (qh, ql), (sgh, sgl), target[:width], target[width : width + 1])
    square = refs[-1]
    square_of(square, relations[ids[bucket]])
    source_into(source_out, state_out.at[0], square, (gh, gl), source[...], source_state[0])
    if len(refs) > 1:
        put_split(refs[:2], source_out[...])


VMEM = pl.BlockSpec(memory_space=pltpu.VMEM)
SMEM = pl.BlockSpec(memory_space=pltpu.SMEM)
HBM = pl.BlockSpec(memory_space=pltpu.HBM)


def in_hbm(x):
    return pltpu.with_memory_space_constraint(x, pltpu.HBM)


def call(kernel, name, args, args_in, outs, scratch=(), flops=0, outs_in=None, aliases=None):
    return pl.pallas_call(
        kernel,
        in_specs=args_in,
        out_specs=outs_in or [VMEM] * len(outs),
        out_shape=[jax.ShapeDtypeStruct(shape, dtype) for shape, dtype in outs],
        scratch_shapes=[pltpu.VMEM(*s) if isinstance(s, tuple) else s for s in scratch],
        input_output_aliases=aliases or {},
        compiler_params=pltpu.CompilerParams(vmem_limit_bytes=VMEM_LIMIT),
        cost_estimate=pl.CostEstimate(flops=flops, transcendentals=0, bytes_accessed=0),
        name=name,
    )(*args)


VMEM_LIMIT = 16 << 20


def shards(source_rows, source_state, target_rows, destination_state, positives, relation_ids, relations):
    buckets, kinds, width = positives.shape[0], relations.shape[0], relations.shape[1]
    if kinds % 2 or buckets % 2 or width % 16:
        raise ValueError("unsupported shapes")
    source, state = source_rows[0, 0], source_state
    target, target_state = target_rows[0, 0], destination_state
    columns, block = source.shape[1], target.shape[1]
    scale = grad_gain / math.sqrt(columns * lax.axis_size("blk") * lax.axis_size("grp"))
    pieces, me = piece_plan()
    me, ids = me[None], relation_ids[:, 0, 0]
    wide, tall = round_up(width, LANES), round_up(width + 1, 8)
    rows = packed_rows(width, kinds, pieces)
    q_pair = [((wide, columns), BF16)] * 2
    sg_pair = [((block, columns), BF16)] * 2
    square = [((wide, wide), F32)]
    moving = [((tall, block), F32)]
    scores = [((block, columns), F32)]
    source_outs = [((width, columns), F32), (source_state.shape, F32)]
    product = 6 * width * width * columns
    updates = buckets // 2
    rel_out, packed_out, y_pair = (relations.shape, F32), ((rows, LANES), F32), [((block, wide), BF16)] * 2
    grads, grads_out = None, ((updates, *relations.shape), F32)
    for update in range(updates):
        bucket, last = 2 * update, update == updates - 1
        if update == 0:
            after, sgh, sgl = call(
                opening_kernel, "opening",
                [me, *(in_hbm(x) for x in (ids, positives, relations, source, target, target_state))], [SMEM] + [HBM] * 6, moving + sg_pair,
                square + q_pair + q_pair + scores + [
                    (relations.shape, F32), (source.shape, F32), (target.shape, F32), (target_state.shape, F32),
                    (positives.shape[1:], jnp.int32), pltpu.SMEM(ids.shape, jnp.int32), pltpu.SemaphoreType.DMA((6,))],
                3 * product)
        else:
            scaled, relations, after, sgh, sgl = call(
                functools.partial(first_kernel, bucket=bucket, pieces=pieces, scale=scale), "first",
                (ids, me, positives, other, relations, *own, xh, xl, target, yh, yl), [SMEM] * 2 + [VMEM] * 10,
                [rel_out, rel_out] + moving + sg_pair, square + q_pair + scores, 3 * product, aliases={5: 0, 6: 1})
        arriving = from_behind(after, "blk", 1)
        args, outs = (ids, relations, source, state, target, sgh, sgl), source_outs + [((width, wide), F32)] + q_pair + q_pair
        if update == 0:
            source, state, grad, qh, ql, xh, xl = call(
                functools.partial(second_kernel, bucket=bucket, place=None), "second",
                args, [SMEM] + [VMEM] * 6, outs, square + q_pair, 4 * product)
        else:
            before = () if grads is None else (grads,)
            source, state, grad, qh, ql, xh, xl, grads = call(
                functools.partial(second_kernel, bucket=bucket, place=update - 1), "second",
                (*args, scaled, *before), [SMEM] + [VMEM] * 7 + [HBM] * len(before), outs + [grads_out],
                square + q_pair + [pltpu.SemaphoreType.DMA((1,))], 4 * product,
                [VMEM] * len(outs) + [HBM], {8: len(outs)} if before else None)
        target = arriving
        packed, sgh, sgl, gh, gl = call(
            functools.partial(third_kernel, bucket=bucket + 1, kinds=kinds, pieces=pieces), "third",
            (ids, me, positives, xh, xl, target, qh, ql, grad), [SMEM] * 2 + [VMEM] * 7,
            [packed_out] + sg_pair + q_pair, scores, 3 * product)

        def close(half, own=None):
            before = tuple(own) if own is not None else () if grads is None else (grads,)
            return call(
                functools.partial(closing_kernel, pieces=pieces, scale=scale, place=updates - 1, half=0 if own is None else 1), "closing",
                (me, half, relations, *before), [SMEM, VMEM, VMEM] + [HBM] * len(before),
                [grads_out, rel_out], [rel_out, rel_out, pltpu.SemaphoreType.DMA((kinds,))],
                product // 4, [HBM, HBM], {3 + i: i for i in range(len(before))})

        own, other, target, source, state, *prepared = sum_everywhere(
            packed,
            lambda *args: call(
                functools.partial(fourth_kernel, bucket=bucket + 1), "fourth",
                (ids, *args), [SMEM] + [VMEM] * len(args), moving + source_outs + ([] if last else q_pair), square, 2 * product),
            (relations, source, state, target, qh, ql, sgh, sgl, gh, gl),
            (lambda target: [target[None, None, :width], target[None, width : width + 1]]) if last else lambda target: call(
                functools.partial(prepare_kernel, width=width), "prepare", (target,), [VMEM], y_pair, (), product // 4),
            close if last else lambda half: call(
                functools.partial(own_kernel, pieces=pieces, scale=scale), "own",
                (me, half, relations), [SMEM, VMEM, VMEM], [rel_out, rel_out], (), product // 4))
        if not last:
            xh, xl, yh, yl = prepared
    grads, relations = close(other, own)
    return (
        source[None, None],
        state,
        *prepared,
        relations,
        grads,
    )


def solution(mesh):
    rows, columns = P("blk", "grp", None, None), P("blk", "grp", None)
    in_specs = (rows, columns, rows, columns, P(None, "blk", "grp", None), P(None, "blk", "grp"), P())
    out_specs = (rows, columns, rows, columns, P(), P())
    return jax.shard_map(shards, mesh=mesh, in_specs=in_specs, out_specs=out_specs, check_vma=False)
```

```python
import functools
import math

import jax
import jax.numpy as jnp
from jax import lax
from jax.experimental import pallas as pl
from jax.experimental.pallas import tpu as pltpu
from jax.sharding import PartitionSpec as P

entity_rate = 0.1
operator_rate = 0.01
grad_gain = 6.0
AXES = ("blk", "grp")
LANES = 128
PART = 256
F32, BF16 = jnp.float32, jnp.bfloat16


def round_up(value, step):
    return -(-value // step) * step


def from_behind(value, axis, steps):
    count = lax.axis_size(axis)
    pairs = [(source, (source + steps) % count) for source in range(count)]
    return lax.ppermute(value, axis, pairs)


def exchange(value, blk_mask, grp_mask):
    blk, grp = lax.axis_size("blk"), lax.axis_size("grp")
    pairs = [(b * grp + g, (b ^ blk_mask) * grp + (g ^ grp_mask)) for b in range(blk) for g in range(grp)]
    return lax.ppermute(value, AXES, pairs)


def group_masks(bits):
    masks = []
    for member in range(1, 1 << len(bits)):
        blk_mask = sum(m for i, (axis, m) in enumerate(bits) if axis == "blk" and member >> i & 1)
        grp_mask = sum(m for i, (axis, m) in enumerate(bits) if axis == "grp" and member >> i & 1)
        masks.append((member, blk_mask, grp_mask))
    return sorted(masks, key=lambda t: -bin(t[0]).count("1"))


def own_member(bits):
    member = jnp.int32(0)
    for i, (axis, m) in enumerate(bits):
        member = member + (((lax.axis_index(axis) // m) % 2) << i)
    return member


def reduce_plan(blk, grp):
    if blk & (blk - 1) or grp & (grp - 1):
        return None
    blk_bits = [("blk", 1 << i) for i in range(blk.bit_length() - 1)]
    grp_bits = [("grp", 1 << i) for i in range(grp.bit_length() - 1)]
    stages = [s for s in (blk_bits[:1], blk_bits[1:3], grp_bits[:2]) if s]
    return (stages, blk_bits[3:] + grp_bits[2:]) if len(stages) > 1 else None


def scatter_sum(value, bits):
    blocks = value.reshape((1 << len(bits), -1) + value.shape[1:])
    total = blocks[0]
    for block in [exchange(blocks[d], mb, mg) for d, mb, mg in group_masks(bits)]:
        total = total + block
    return total


def gather(value, bits):
    arrived = {d: exchange(value, mb, mg) for d, mb, mg in group_masks(bits)}
    arrived[0] = value
    return jnp.concatenate([arrived[d] for d in range(len(arrived))], axis=0)


def piece_plan():
    plan = reduce_plan(lax.axis_size("blk"), lax.axis_size("grp"))
    if plan is None:
        return 1, jnp.int32(0)
    count, me = 1, jnp.int32(0)
    for stage in plan[0]:
        count <<= len(stage)
        me = (me << len(stage)) + own_member(stage)
    return count, me


def sum_everywhere(packed, work, args, work_on_arrival, work_on_half):
    plan = reduce_plan(lax.axis_size("blk"), lax.axis_size("grp"))
    if plan is None:
        after, *rest = work(*args)
        arriving = from_behind(after, "blk", 1)
        total = lax.psum(packed, AXES)
        middle = total.shape[0] // 2
        own, other = work_on_half(total[:middle]), total[middle:]
        return own, other, arriving, *rest, *work_on_arrival(arriving)
    stages, singles = plan
    for place, stage in enumerate(stages):
        if place == 1:
            packed, args = lax.optimization_barrier((packed, args))
            after, *rest = work(*args)
        packed = scatter_sum(packed, stage)
        if place == 1:
            packed, after = lax.optimization_barrier((packed, after))
            arriving = from_behind(after, "blk", 1)
    for axis, mask in singles:
        packed = packed + exchange(packed, mask if axis == "blk" else 0, mask if axis == "grp" else 0)
    for place, stage in reversed(list(enumerate(stages))[1:]):
        if place == 1:
            packed, arriving = lax.optimization_barrier((packed, arriving))
            rest += work_on_arrival(arriving)
        packed = gather(packed, stage)
        if place == 1:
            packed, rest = lax.optimization_barrier((packed, rest))
    other = exchange(packed, *group_masks(stages[0])[0][1:])
    return work_on_half(packed), other, arriving, *rest


NN = (((1,), (0,)), ((), ()))
NT = (((1,), (1,)), ((), ()))


def dot3(ah, al, bh, bl, dims):
    one = functools.partial(lax.dot_general, dimension_numbers=dims, preferred_element_type=F32)
    return one(ah, bh) + (one(ah, bl) + one(al, bh))


def split(x):
    high = x.astype(BF16)
    return high, (x - high.astype(F32)).astype(BF16)


def put_split(refs, x):
    rows = x.shape[0]
    refs[0][:rows], refs[1][:rows] = split(x)
    if rows < refs[0].shape[0]:
        blank = jnp.zeros((refs[0].shape[0] - rows, x.shape[1]), BF16)
        refs[0][rows:], refs[1][rows:] = blank, blank


def both(refs, rows=None):
    return (refs[0][...], refs[1][...]) if rows is None else (refs[0][:rows], refs[1][:rows])


def pad_rows(x, rows):
    return jnp.concatenate([x, jnp.zeros((rows - x.shape[0], x.shape[1]), x.dtype)], axis=0)


def square_of(pad_ref, matrix):
    width = matrix.shape[0]
    pad_ref[...] = jnp.zeros(pad_ref.shape, F32)
    pad_ref[:width, :width] = matrix


def parts_of(size):
    return [slice(start, min(start + PART, size)) for start in range(0, size, PART)]


def columns_of(refs, part, rows=None):
    return (refs[0][:rows, part], refs[1][:rows, part])


def split_columns(refs, compute):
    for part in parts_of(refs[0].shape[1]):
        high, low = split(compute(part))
        rows = high.shape[0]
        refs[0][:rows, part], refs[1][:rows, part] = high, low
        if rows < refs[0].shape[0]:
            blank = jnp.zeros((refs[0].shape[0] - rows, high.shape[1]), BF16)
            refs[0][rows:, part], refs[1][rows:, part] = blank, blank


def turned_halves(square_ref, width):
    return split(square_ref[...].T[:width])


def queries_into(q_refs, square_ref, x_refs, width, turned=None):
    turned = turned_halves(square_ref, width) if turned is None else turned
    split_columns(q_refs, lambda part: dot3(*turned, *columns_of(x_refs, part), NN))


def score_grad_into(sg_refs, scores, q_refs, target_turned, partner):
    for part in parts_of(scores.shape[1]):
        scores[:, part] = dot3(*target_turned, *columns_of(q_refs, part), NN)

    def gradient(part):
        score = scores[:, part]
        expo = jnp.exp(score - jnp.max(score, axis=0, keepdims=True))
        chance = expo * (1.0 / jnp.sum(expo, axis=0, keepdims=True))
        row = lax.broadcasted_iota(jnp.int32, score.shape, 0)
        return chance - jnp.where(row == partner[:, part], 1.0, 0.0)

    split_columns(sg_refs, gradient)


def adagrad(values, state, gradient):
    state_new = state + jnp.sum(gradient * gradient, axis=0, keepdims=True) * (1.0 / values.shape[0])
    return values - gradient * (entity_rate / jnp.sqrt(state_new)), state_new


def target_into(out_ref, q_refs, sg_refs, target, state):
    width = target.shape[0]
    for part in parts_of(target.shape[1]):
        gradient = dot3(*both(q_refs, width), sg_refs[0][part], sg_refs[1][part], NT)
        out_ref[:width, part], out_ref[width : width + 1, part] = adagrad(target[:, part], state[:, part], gradient)
    rest = out_ref.shape[0] - width - 1
    out_ref[width + 1 :] = jnp.zeros((rest, target.shape[1]), F32)


def query_grad_into(g_refs, sg_refs, target):
    halves = split(target)
    split_columns(g_refs, lambda part: dot3(*halves, *columns_of(sg_refs, part), NN))


def operator_grad(x_halves, g_refs):
    return jnp.concatenate(
        [dot3(*x_halves, g_refs[0][part], g_refs[1][part], NT) for part in parts_of(g_refs[0].shape[0])], axis=1)


def source_into(x_out, state_out, square_ref, g_refs, source, state):
    halves = split(square_ref[: source.shape[0]])
    for part in parts_of(source.shape[1]):
        gradient = dot3(*halves, *columns_of(g_refs, part), NN)
        x_out[:, part], state_out[:, part] = adagrad(source[:, part], state[:, part], gradient)


class Pieces:
    def __init__(self, ref, me, count):
        self.ref, self.me, self.rows = ref, me, ref.shape[0] // count

    def runs(self, start, stop):
        while start < stop:
            piece, place = divmod(start, self.rows)
            end = min(stop, (piece + 1) * self.rows)
            first = pl.multiple_of((self.me ^ piece) * self.rows + place, 8)
            yield start, end, pl.ds(first, end - start)
            start = end

    def put(self, start, value):
        for first, end, here in self.runs(start, start + value.shape[0]):
            self.ref[here] = value[first - start : end - start]

    def get(self, start, size):
        found = [self.ref[here] for _, _, here in self.runs(start, start + size)]
        return jnp.concatenate(found, axis=0) if len(found) > 1 else found[0]


def pack_into(packed, parts, kinds):
    width = parts[0][1].shape[0]
    full, tail = divmod(width, LANES)
    span, rows = tail_span(width), packed.ref.shape[0] // kinds
    for kind in range(kinds):
        total = sum(jnp.where(index == kind, part, 0.0) for index, part in parts)
        start = kind * rows
        for block in range(full):
            packed.put(start, total[:, block * LANES : (block + 1) * LANES])
            start += width
        if tail:
            ends, packed_tail = total[:, full * LANES :], None
            for place, first in enumerate(range(0, width, span)):
                moved = ends[first : first + span]
                moved = moved if moved.shape[0] == span else pad_rows(moved, span)
                moved = pltpu.roll(moved, place * tail, 1) if place else moved
                packed_tail = moved if packed_tail is None else packed_tail + moved
            packed.put(start, packed_tail)
            start += span
        if start < (kind + 1) * rows:
            packed.put(start, jnp.zeros(((kind + 1) * rows - start, LANES), F32))


def tail_span(width):
    tail = width % LANES
    return round_up(-(-width // (LANES // tail)), 8) if tail else 0


def packed_rows(width, kinds, pieces):
    return kinds * round_up((width // LANES) * width + tail_span(width), 8 * pieces)


def unpack(packed, place_of_kind, kinds, scaled_out, kind, scale):
    width, (full, tail) = scaled_out.shape[1], divmod(scaled_out.shape[1], LANES)
    start = place_of_kind * (packed.ref.shape[0] // kinds)
    for block in range(full):
        scaled_out[kind, :, block * LANES : (block + 1) * LANES] = scale * packed.get(start, width)
        start += width
    if tail:
        span = tail_span(width)
        ends = packed.get(start, span)
        for place, first in enumerate(range(0, width, span)):
            rows = min(span, width - first)
            moved = pltpu.roll(ends, LANES - place * tail, 1) if place else ends
            scaled_out[kind, first : first + rows, full * LANES :] = scale * moved[:rows, :tail]


def opening_kernel(me, ids, partners, relations, source, target, target_state, target_out, sgh, sgl, square, xh, xl, qh, ql, scores, matrix, source_in, target_in, state_in, partners_in, ids_in, sems):
    width = source.shape[0]
    pairs = ((ids, ids_in), (relations, matrix), (source, source_in), (target, target_in), (target_state, state_in), (partners.at[0], partners_in))
    loads = [pltpu.make_async_copy(here, there, sems.at[place]) for place, (here, there) in enumerate(pairs)]
    for load in loads:
        load.start()
    loads[0].wait()
    loads[1].wait()
    square_of(square, matrix[ids_in[0]])
    halves = turned_halves(square, width)
    loads[2].wait()
    put_split((xh, xl), source_in[...])
    for load in loads[3:]:
        load.wait()
    body = target_in[...]
    turned = split(pad_rows(body, qh.shape[0]).T)
    queries_into((qh, ql), square, (xh, xl), width, halves)
    score_grad_into((sgh, sgl), scores, (qh, ql), turned, partners_in[0])
    target_into(target_out, (qh, ql), (sgh, sgl), body, state_in[0])


def prepare_kernel(target, yh, yl, *, width):
    yh[...], yl[...] = split(pad_rows(target[:width], yh.shape[1]).T)


def renew(me, packed, relations, scaled, renewed, pieces, scale, half, done=None):
    kinds, count = relations.shape[0] // 2, max(pieces // 2, 1)
    for place in range(kinds):
        kind = ((me[0] // count) ^ half if pieces > 1 else half) * kinds + place
        unpack(Pieces(packed, me[0] % count, count), place, kinds, scaled, kind, scale)
        renewed[kind] = relations[kind] - operator_rate * scaled[kind]
        if done is not None:
            done(place, kind)


def own_kernel(me, packed, relations, scaled, renewed, *, pieces, scale):
    renew(me, packed, relations, scaled, renewed, pieces, scale, 0)


def first_kernel(ids, me, partners, packed, relations, own_scaled, own_renewed, xh, xl, target, yh, yl, scaled, renewed, target_out, sgh, sgl, square, qh, ql, scores, *, bucket, pieces, scale):
    width = relations.shape[1]
    renew(me, packed, relations, scaled, renewed, pieces, scale, 1)
    square_of(square, renewed[ids[bucket]])
    queries_into((qh, ql), square, (xh, xl), width)
    score_grad_into((sgh, sgl), scores, (qh, ql), both((yh, yl)), partners[bucket, 0])
    target_into(target_out, (qh, ql), (sgh, sgl), target[:width], target[width : width + 1])


def closing_kernel(me, packed, relations, *refs, pieces, scale, place, half):
    grads_out, relations_out, scaled, renewed, sems = refs[-5:]
    stores = []

    def store(slot, kind):
        for here, there in ((scaled, grads_out.at[place]), (renewed, relations_out)):
            stores.append(pltpu.make_async_copy(here.at[kind], there.at[kind], sems.at[len(stores)]))
            stores[-1].start()

    renew(me, packed, relations, scaled, renewed, pieces, scale, half, store)
    for copy in stores:
        copy.wait()


def second_kernel(ids, relations, source, source_state, target, sgh, sgl, *refs, bucket, place):
    if place is None:
        source_out, state_out, grad_out, qh, ql, xh, xl, square, gh, gl = refs
    else:
        scaled, *refs = refs
        source_out, state_out, grad_out, qh, ql, xh, xl, grads_out, square, gh, gl, sem = refs[1 if place else 0 :]
        store = pltpu.make_async_copy(scaled, grads_out.at[place], sem.at[0])
        store.start()
    width = source.shape[0]
    query_grad_into((gh, gl), (sgh, sgl), target[:width])
    put_split((xh, xl), source[...])
    grad_out[...] = operator_grad(both((xh, xl), width), (gh, gl))
    square_of(square, relations[ids[bucket]])
    source_into(source_out, state_out.at[0], square, (gh, gl), source[...], source_state[0])
    square_of(square, relations[ids[bucket + 1]])
    put_split((xh, xl), source_out[...])
    queries_into((qh, ql), square, (xh, xl), width)
    if place is not None:
        store.wait()


def third_kernel(ids, me, partners, xh, xl, target, qh, ql, grad_before, packed, sgh, sgl, gh, gl, scores, *, bucket, kinds, pieces):
    width = grad_before.shape[0]
    body = target[:width]
    score_grad_into((sgh, sgl), scores, (qh, ql), split(pad_rows(body, qh.shape[0]).T), partners[bucket, 0])
    query_grad_into((gh, gl), (sgh, sgl), body)
    grad = operator_grad(both((xh, xl), width), (gh, gl))
    pack_into(Pieces(packed, me[0], pieces), ((ids[bucket - 1], grad_before[...]), (ids[bucket], grad)), kinds)


def fourth_kernel(ids, relations, source, source_state, target, qh, ql, sgh, sgl, gh, gl, target_out, source_out, state_out, *refs, bucket):
    width = source.shape[0]
    target_into(target_out, (qh, ql), (sgh, sgl), target[:width], target[width : width + 1])
    square = refs[-1]
    square_of(square, relations[ids[bucket]])
    source_into(source_out, state_out.at[0], square, (gh, gl), source[...], source_state[0])
    if len(refs) > 1:
        put_split(refs[:2], source_out[...])


VMEM = pl.BlockSpec(memory_space=pltpu.VMEM)
SMEM = pl.BlockSpec(memory_space=pltpu.SMEM)
HBM = pl.BlockSpec(memory_space=pltpu.HBM)


def in_hbm(x):
    return pltpu.with_memory_space_constraint(x, pltpu.HBM)


def call(kernel, name, args, args_in, outs, scratch=(), flops=0, outs_in=None, aliases=None):
    return pl.pallas_call(
        kernel,
        in_specs=args_in,
        out_specs=outs_in or [VMEM] * len(outs),
        out_shape=[jax.ShapeDtypeStruct(shape, dtype) for shape, dtype in outs],
        scratch_shapes=[pltpu.VMEM(*s) if isinstance(s, tuple) else s for s in scratch],
        input_output_aliases=aliases or {},
        compiler_params=pltpu.CompilerParams(vmem_limit_bytes=VMEM_LIMIT),
        cost_estimate=pl.CostEstimate(flops=flops, transcendentals=0, bytes_accessed=0),
        name=name,
    )(*args)


VMEM_LIMIT = 16 << 20


def shards(source_rows, source_state, target_rows, destination_state, positives, relation_ids, relations):
    buckets, kinds, width = positives.shape[0], relations.shape[0], relations.shape[1]
    if kinds % 2 or buckets % 2 or width % 16:
        raise ValueError("unsupported shapes")
    source, state = source_rows[0, 0], source_state
    target, target_state = target_rows[0, 0], destination_state
    columns, block = source.shape[1], target.shape[1]
    scale = grad_gain / math.sqrt(columns * lax.axis_size("blk") * lax.axis_size("grp"))
    pieces, me = piece_plan()
    me, ids = me[None], relation_ids[:, 0, 0]
    wide, tall = round_up(width, LANES), round_up(width + 1, 8)
    rows = packed_rows(width, kinds, pieces)
    q_pair = [((wide, columns), BF16)] * 2
    sg_pair = [((block, columns), BF16)] * 2
    square = [((wide, wide), F32)]
    moving = [((tall, block), F32)]
    scores = [((block, columns), F32)]
    source_outs = [((width, columns), F32), (source_state.shape, F32)]
    product = 6 * width * width * columns
    updates = buckets // 2
    rel_out, packed_out, y_pair = (relations.shape, F32), ((rows, LANES), F32), [((block, wide), BF16)] * 2
    grads, grads_out = None, ((updates, *relations.shape), F32)
    for update in range(updates):
        bucket, last = 2 * update, update == updates - 1
        if update == 0:
            after, sgh, sgl = call(
                opening_kernel, "opening",
                [me, *(in_hbm(x) for x in (ids, positives, relations, source, target, target_state))], [SMEM] + [HBM] * 6, moving + sg_pair,
                square + q_pair + q_pair + scores + [
                    (relations.shape, F32), (source.shape, F32), (target.shape, F32), (target_state.shape, F32),
                    (positives.shape[1:], jnp.int32), pltpu.SMEM(ids.shape, jnp.int32), pltpu.SemaphoreType.DMA((6,))],
                3 * product)
        else:
            scaled, relations, after, sgh, sgl = call(
                functools.partial(first_kernel, bucket=bucket, pieces=pieces, scale=scale), "first",
                (ids, me, positives, other, relations, *own, xh, xl, target, yh, yl), [SMEM] * 2 + [VMEM] * 10,
                [rel_out, rel_out] + moving + sg_pair, square + q_pair + scores, 3 * product, aliases={5: 0, 6: 1})
        arriving = from_behind(after, "blk", 1)
        args, outs = (ids, relations, source, state, target, sgh, sgl), source_outs + [((width, wide), F32)] + q_pair + q_pair
        if update == 0:
            source, state, grad, qh, ql, xh, xl = call(
                functools.partial(second_kernel, bucket=bucket, place=None), "second",
                args, [SMEM] + [VMEM] * 6, outs, square + q_pair, 4 * product)
        else:
            before = () if grads is None else (grads,)
            source, state, grad, qh, ql, xh, xl, grads = call(
                functools.partial(second_kernel, bucket=bucket, place=update - 1), "second",
                (*args, scaled, *before), [SMEM] + [VMEM] * 7 + [HBM] * len(before), outs + [grads_out],
                square + q_pair + [pltpu.SemaphoreType.DMA((1,))], 4 * product,
                [VMEM] * len(outs) + [HBM], {8: len(outs)} if before else None)
        target = arriving
        packed, sgh, sgl, gh, gl = call(
            functools.partial(third_kernel, bucket=bucket + 1, kinds=kinds, pieces=pieces), "third",
            (ids, me, positives, xh, xl, target, qh, ql, grad), [SMEM] * 2 + [VMEM] * 7,
            [packed_out] + sg_pair + q_pair, scores, 3 * product)

        def close(half, own=None):
            before = tuple(own) if own is not None else () if grads is None else (grads,)
            return call(
                functools.partial(closing_kernel, pieces=pieces, scale=scale, place=updates - 1, half=0 if own is None else 1), "closing",
                (me, half, relations, *before), [SMEM, VMEM, VMEM] + [HBM] * len(before),
                [grads_out, rel_out], [rel_out, rel_out, pltpu.SemaphoreType.DMA((kinds,))],
                product // 4, [HBM, HBM], {3 + i: i for i in range(len(before))})

        own, other, target, source, state, *prepared = sum_everywhere(
            packed,
            lambda *args: call(
                functools.partial(fourth_kernel, bucket=bucket + 1), "fourth",
                (ids, *args), [SMEM] + [VMEM] * len(args), moving + source_outs + ([] if last else q_pair), square, 2 * product),
            (relations, source, state, target, qh, ql, sgh, sgl, gh, gl),
            (lambda target: [target[None, None, :width], target[None, width : width + 1]]) if last else lambda target: call(
                functools.partial(prepare_kernel, width=width), "prepare", (target,), [VMEM], y_pair, (), product // 4),
            close if last else lambda half: call(
                functools.partial(own_kernel, pieces=pieces, scale=scale), "own",
                (me, half, relations), [SMEM, VMEM, VMEM], [rel_out, rel_out], (), product // 4))
        if not last:
            xh, xl, yh, yl = prepared
    grads, relations = close(other, own)
    return (
        source[None, None],
        state,
        *prepared,
        relations,
        grads,
    )


def solution(mesh):
    rows, columns = P("blk", "grp", None, None), P("blk", "grp", None)
    in_specs = (rows, columns, rows, columns, P(None, "blk", "grp", None), P(None, "blk", "grp"), P())
    out_specs = (rows, columns, rows, columns, P(), P())
    return jax.shard_map(shards, mesh=mesh, in_specs=in_specs, out_specs=out_specs, check_vma=False)
```

```python
import functools
import math

import jax
import jax.numpy as jnp
from jax import lax
from jax.experimental import pallas as pl
from jax.experimental.pallas import tpu as pltpu
from jax.sharding import PartitionSpec as P

entity_rate = 0.1
operator_rate = 0.01
grad_gain = 6.0
AXES = ("blk", "grp")
LANES = 128
PART = 256
F32, BF16 = jnp.float32, jnp.bfloat16


def round_up(value, step):
    return -(-value // step) * step


def from_behind(value, axis, steps):
    count = lax.axis_size(axis)
    pairs = [(source, (source + steps) % count) for source in range(count)]
    return lax.ppermute(value, axis, pairs)


def exchange(value, blk_mask, grp_mask):
    blk, grp = lax.axis_size("blk"), lax.axis_size("grp")
    pairs = [(b * grp + g, (b ^ blk_mask) * grp + (g ^ grp_mask)) for b in range(blk) for g in range(grp)]
    return lax.ppermute(value, AXES, pairs)


def group_masks(bits):
    masks = []
    for member in range(1, 1 << len(bits)):
        blk_mask = sum(m for i, (axis, m) in enumerate(bits) if axis == "blk" and member >> i & 1)
        grp_mask = sum(m for i, (axis, m) in enumerate(bits) if axis == "grp" and member >> i & 1)
        masks.append((member, blk_mask, grp_mask))
    return sorted(masks, key=lambda t: -bin(t[0]).count("1"))


def own_member(bits):
    member = jnp.int32(0)
    for i, (axis, m) in enumerate(bits):
        member = member + (((lax.axis_index(axis) // m) % 2) << i)
    return member


def reduce_plan(blk, grp):
    if blk & (blk - 1) or grp & (grp - 1):
        return None
    blk_bits = [("blk", 1 << i) for i in range(blk.bit_length() - 1)]
    grp_bits = [("grp", 1 << i) for i in range(grp.bit_length() - 1)]
    stages = [s for s in (blk_bits[:1], blk_bits[1:3], grp_bits[:2]) if s]
    return (stages, blk_bits[3:] + grp_bits[2:]) if len(stages) > 1 else None


def scatter_sum(value, bits):
    blocks = value.reshape((1 << len(bits), -1) + value.shape[1:])
    total = blocks[0]
    for block in [exchange(blocks[d], mb, mg) for d, mb, mg in group_masks(bits)]:
        total = total + block
    return total


def gather(value, bits):
    arrived = {d: exchange(value, mb, mg) for d, mb, mg in group_masks(bits)}
    arrived[0] = value
    return jnp.concatenate([arrived[d] for d in range(len(arrived))], axis=0)


def piece_plan():
    plan = reduce_plan(lax.axis_size("blk"), lax.axis_size("grp"))
    if plan is None:
        return 1, jnp.int32(0)
    count, me = 1, jnp.int32(0)
    for stage in plan[0]:
        count <<= len(stage)
        me = (me << len(stage)) + own_member(stage)
    return count, me


def sum_everywhere(packed, work, args, work_on_arrival, work_on_half):
    plan = reduce_plan(lax.axis_size("blk"), lax.axis_size("grp"))
    if plan is None:
        after, *rest = work(*args)
        arriving = from_behind(after, "blk", 1)
        total = lax.psum(packed, AXES)
        middle = total.shape[0] // 2
        own, other = work_on_half(total[:middle]), total[middle:]
        return own, other, arriving, *rest, *work_on_arrival(arriving)
    stages, singles = plan
    for place, stage in enumerate(stages):
        if place == 1:
            packed, args = lax.optimization_barrier((packed, args))
            after, *rest = work(*args)
        packed = scatter_sum(packed, stage)
        if place == 1:
            packed, after = lax.optimization_barrier((packed, after))
            arriving = from_behind(after, "blk", 1)
    for axis, mask in singles:
        packed = packed + exchange(packed, mask if axis == "blk" else 0, mask if axis == "grp" else 0)
    for place, stage in reversed(list(enumerate(stages))[1:]):
        if place == 1:
            packed, arriving = lax.optimization_barrier((packed, arriving))
            rest += work_on_arrival(arriving)
        packed = gather(packed, stage)
        if place == 1:
            packed, rest = lax.optimization_barrier((packed, rest))
    other = exchange(packed, *group_masks(stages[0])[0][1:])
    return work_on_half(packed), other, arriving, *rest


NN = (((1,), (0,)), ((), ()))
NT = (((1,), (1,)), ((), ()))


def dot3(ah, al, bh, bl, dims):
    one = functools.partial(lax.dot_general, dimension_numbers=dims, preferred_element_type=F32)
    return one(ah, bh) + (one(ah, bl) + one(al, bh))


def split(x):
    high = x.astype(BF16)
    return high, (x - high.astype(F32)).astype(BF16)


def put_split(refs, x):
    rows = x.shape[0]
    refs[0][:rows], refs[1][:rows] = split(x)
    if rows < refs[0].shape[0]:
        blank = jnp.zeros((refs[0].shape[0] - rows, x.shape[1]), BF16)
        refs[0][rows:], refs[1][rows:] = blank, blank


def both(refs, rows=None):
    return (refs[0][...], refs[1][...]) if rows is None else (refs[0][:rows], refs[1][:rows])


def pad_rows(x, rows):
    return jnp.concatenate([x, jnp.zeros((rows - x.shape[0], x.shape[1]), x.dtype)], axis=0)


def square_of(pad_ref, matrix):
    width = matrix.shape[0]
    pad_ref[...] = jnp.zeros(pad_ref.shape, F32)
    pad_ref[:width, :width] = matrix


def parts_of(size):
    return [slice(start, min(start + PART, size)) for start in range(0, size, PART)]


def columns_of(refs, part, rows=None):
    return (refs[0][:rows, part], refs[1][:rows, part])


def split_columns(refs, compute):
    for part in parts_of(refs[0].shape[1]):
        high, low = split(compute(part))
        rows = high.shape[0]
        refs[0][:rows, part], refs[1][:rows, part] = high, low
        if rows < refs[0].shape[0]:
            blank = jnp.zeros((refs[0].shape[0] - rows, high.shape[1]), BF16)
            refs[0][rows:, part], refs[1][rows:, part] = blank, blank


def turned_halves(square_ref, width):
    return split(square_ref[...].T[:width])


def queries_into(q_refs, square_ref, x_refs, width, turned=None):
    turned = turned_halves(square_ref, width) if turned is None else turned
    split_columns(q_refs, lambda part: dot3(*turned, *columns_of(x_refs, part), NN))


def score_grad_into(sg_refs, scores, q_refs, target_turned, partner):
    for part in parts_of(scores.shape[1]):
        scores[:, part] = dot3(*target_turned, *columns_of(q_refs, part), NN)

    def gradient(part):
        score = scores[:, part]
        expo = jnp.exp(score - jnp.max(score, axis=0, keepdims=True))
        chance = expo * (1.0 / jnp.sum(expo, axis=0, keepdims=True))
        row = lax.broadcasted_iota(jnp.int32, score.shape, 0)
        return chance - jnp.where(row == partner[:, part], 1.0, 0.0)

    split_columns(sg_refs, gradient)


def adagrad(values, state, gradient):
    state_new = state + jnp.sum(gradient * gradient, axis=0, keepdims=True) * (1.0 / values.shape[0])
    return values - gradient * (entity_rate / jnp.sqrt(state_new)), state_new


def target_into(out_ref, q_refs, sg_refs, target, state):
    width = target.shape[0]
    for part in parts_of(target.shape[1]):
        gradient = dot3(*both(q_refs, width), sg_refs[0][part], sg_refs[1][part], NT)
        out_ref[:width, part], out_ref[width : width + 1, part] = adagrad(target[:, part], state[:, part], gradient)
    rest = out_ref.shape[0] - width - 1
    out_ref[width + 1 :] = jnp.zeros((rest, target.shape[1]), F32)


def query_grad_into(g_refs, sg_refs, target):
    halves = split(target)
    split_columns(g_refs, lambda part: dot3(*halves, *columns_of(sg_refs, part), NN))


def operator_grad(x_halves, g_refs):
    return jnp.concatenate(
        [dot3(*x_halves, g_refs[0][part], g_refs[1][part], NT) for part in parts_of(g_refs[0].shape[0])], axis=1)


def source_into(x_out, state_out, square_ref, g_refs, source, state):
    halves = split(square_ref[: source.shape[0]])
    for part in parts_of(source.shape[1]):
        gradient = dot3(*halves, *columns_of(g_refs, part), NN)
        x_out[:, part], state_out[:, part] = adagrad(source[:, part], state[:, part], gradient)


class Pieces:
    def __init__(self, ref, me, count):
        self.ref, self.me, self.rows = ref, me, ref.shape[0] // count

    def runs(self, start, stop):
        while start < stop:
            piece, place = divmod(start, self.rows)
            end = min(stop, (piece + 1) * self.rows)
            first = pl.multiple_of((self.me ^ piece) * self.rows + place, 8)
            yield start, end, pl.ds(first, end - start)
            start = end

    def put(self, start, value):
        for first, end, here in self.runs(start, start + value.shape[0]):
            self.ref[here] = value[first - start : end - start]

    def get(self, start, size):
        found = [self.ref[here] for _, _, here in self.runs(start, start + size)]
        return jnp.concatenate(found, axis=0) if len(found) > 1 else found[0]


def pack_into(packed, parts, kinds):
    width = parts[0][1].shape[0]
    full, tail = divmod(width, LANES)
    span, rows = tail_span(width), packed.ref.shape[0] // kinds
    for kind in range(kinds):
        total = sum(jnp.where(index == kind, part, 0.0) for index, part in parts)
        start = kind * rows
        for block in range(full):
            packed.put(start, total[:, block * LANES : (block + 1) * LANES])
            start += width
        if tail:
            ends, packed_tail = total[:, full * LANES :], None
            for place, first in enumerate(range(0, width, span)):
                moved = ends[first : first + span]
                moved = moved if moved.shape[0] == span else pad_rows(moved, span)
                moved = pltpu.roll(moved, place * tail, 1) if place else moved
                packed_tail = moved if packed_tail is None else packed_tail + moved
            packed.put(start, packed_tail)
            start += span
        if start < (kind + 1) * rows:
            packed.put(start, jnp.zeros(((kind + 1) * rows - start, LANES), F32))


def tail_span(width):
    tail = width % LANES
    return round_up(-(-width // (LANES // tail)), 8) if tail else 0


def packed_rows(width, kinds, pieces):
    return kinds * round_up((width // LANES) * width + tail_span(width), 8 * pieces)


def unpack(packed, place_of_kind, kinds, scaled_out, kind, scale):
    width, (full, tail) = scaled_out.shape[1], divmod(scaled_out.shape[1], LANES)
    start = place_of_kind * (packed.ref.shape[0] // kinds)
    for block in range(full):
        scaled_out[kind, :, block * LANES : (block + 1) * LANES] = scale * packed.get(start, width)
        start += width
    if tail:
        span = tail_span(width)
        ends = packed.get(start, span)
        for place, first in enumerate(range(0, width, span)):
            rows = min(span, width - first)
            moved = pltpu.roll(ends, LANES - place * tail, 1) if place else ends
            scaled_out[kind, first : first + rows, full * LANES :] = scale * moved[:rows, :tail]


def opening_kernel(me, ids, partners, relations, source, target, target_state, target_out, sgh, sgl, square, xh, xl, qh, ql, scores, matrix, source_in, target_in, state_in, partners_in, ids_in, sems):
    width = source.shape[0]
    pairs = ((ids, ids_in), (relations, matrix), (target, target_in), (source, source_in), (target_state, state_in), (partners.at[0], partners_in))
    loads = [pltpu.make_async_copy(here, there, sems.at[place]) for place, (here, there) in enumerate(pairs)]
    for load in loads:
        load.start()
    loads[0].wait()
    loads[1].wait()
    square_of(square, matrix[ids_in[0]])
    halves = turned_halves(square, width)
    loads[2].wait()
    body = target_in[...]
    turned = split(pad_rows(body, qh.shape[0]).T)
    for load in loads[3:]:
        load.wait()
    put_split((xh, xl), source_in[...])
    queries_into((qh, ql), square, (xh, xl), width, halves)
    score_grad_into((sgh, sgl), scores, (qh, ql), turned, partners_in[0])
    target_into(target_out, (qh, ql), (sgh, sgl), body, state_in[0])


def prepare_kernel(target, yh, yl, *, width):
    yh[...], yl[...] = split(pad_rows(target[:width], yh.shape[1]).T)


def renew(me, packed, relations, scaled, renewed, pieces, scale, half, done=None):
    kinds, count = relations.shape[0] // 2, max(pieces // 2, 1)
    for place in range(kinds):
        kind = ((me[0] // count) ^ half if pieces > 1 else half) * kinds + place
        unpack(Pieces(packed, me[0] % count, count), place, kinds, scaled, kind, scale)
        renewed[kind] = relations[kind] - operator_rate * scaled[kind]
        if done is not None:
            done(place, kind)


def own_kernel(me, packed, relations, scaled, renewed, *, pieces, scale):
    renew(me, packed, relations, scaled, renewed, pieces, scale, 0)


def first_kernel(ids, me, partners, packed, relations, own_scaled, own_renewed, xh, xl, target, yh, yl, scaled, renewed, target_out, sgh, sgl, square, qh, ql, scores, *, bucket, pieces, scale):
    width = relations.shape[1]
    renew(me, packed, relations, scaled, renewed, pieces, scale, 1)
    square_of(square, renewed[ids[bucket]])
    queries_into((qh, ql), square, (xh, xl), width)
    score_grad_into((sgh, sgl), scores, (qh, ql), both((yh, yl)), partners[bucket, 0])
    target_into(target_out, (qh, ql), (sgh, sgl), target[:width], target[width : width + 1])


def closing_kernel(me, packed, relations, *refs, pieces, scale, place, half):
    grads_out, relations_out, scaled, renewed, sems = refs[-5:]
    stores = []

    def store(slot, kind):
        for here, there in ((scaled, grads_out.at[place]), (renewed, relations_out)):
            stores.append(pltpu.make_async_copy(here.at[kind], there.at[kind], sems.at[len(stores)]))
            stores[-1].start()

    renew(me, packed, relations, scaled, renewed, pieces, scale, half, store)
    for copy in stores:
        copy.wait()


def second_kernel(ids, relations, source, source_state, target, sgh, sgl, *refs, bucket, place):
    if place is None:
        source_out, state_out, grad_out, qh, ql, xh, xl, square, gh, gl = refs
    else:
        scaled, *refs = refs
        source_out, state_out, grad_out, qh, ql, xh, xl, grads_out, square, gh, gl, sem = refs[1 if place else 0 :]
        store = pltpu.make_async_copy(scaled, grads_out.at[place], sem.at[0])
        store.start()
    width = source.shape[0]
    query_grad_into((gh, gl), (sgh, sgl), target[:width])
    put_split((xh, xl), source[...])
    grad_out[...] = operator_grad(both((xh, xl), width), (gh, gl))
    square_of(square, relations[ids[bucket]])
    source_into(source_out, state_out.at[0], square, (gh, gl), source[...], source_state[0])
    square_of(square, relations[ids[bucket + 1]])
    put_split((xh, xl), source_out[...])
    queries_into((qh, ql), square, (xh, xl), width)
    if place is not None:
        store.wait()


def third_kernel(ids, me, partners, xh, xl, target, qh, ql, grad_before, packed, sgh, sgl, gh, gl, scores, *, bucket, kinds, pieces):
    width = grad_before.shape[0]
    body = target[:width]
    score_grad_into((sgh, sgl), scores, (qh, ql), split(pad_rows(body, qh.shape[0]).T), partners[bucket, 0])
    query_grad_into((gh, gl), (sgh, sgl), body)
    grad = operator_grad(both((xh, xl), width), (gh, gl))
    pack_into(Pieces(packed, me[0], pieces), ((ids[bucket - 1], grad_before[...]), (ids[bucket], grad)), kinds)


def fourth_kernel(ids, relations, source, source_state, target, qh, ql, sgh, sgl, gh, gl, target_out, source_out, state_out, *refs, bucket):
    width = source.shape[0]
    target_into(target_out, (qh, ql), (sgh, sgl), target[:width], target[width : width + 1])
    square = refs[-1]
    square_of(square, relations[ids[bucket]])
    source_into(source_out, state_out.at[0], square, (gh, gl), source[...], source_state[0])
    if len(refs) > 1:
        put_split(refs[:2], source_out[...])


VMEM = pl.BlockSpec(memory_space=pltpu.VMEM)
SMEM = pl.BlockSpec(memory_space=pltpu.SMEM)
HBM = pl.BlockSpec(memory_space=pltpu.HBM)


def in_hbm(x):
    return pltpu.with_memory_space_constraint(x, pltpu.HBM)


def call(kernel, name, args, args_in, outs, scratch=(), flops=0, outs_in=None, aliases=None):
    return pl.pallas_call(
        kernel,
        in_specs=args_in,
        out_specs=outs_in or [VMEM] * len(outs),
        out_shape=[jax.ShapeDtypeStruct(shape, dtype) for shape, dtype in outs],
        scratch_shapes=[pltpu.VMEM(*s) if isinstance(s, tuple) else s for s in scratch],
        input_output_aliases=aliases or {},
        compiler_params=pltpu.CompilerParams(vmem_limit_bytes=VMEM_LIMIT),
        cost_estimate=pl.CostEstimate(flops=flops, transcendentals=0, bytes_accessed=0),
        name=name,
    )(*args)


VMEM_LIMIT = 16 << 20


def shards(source_rows, source_state, target_rows, destination_state, positives, relation_ids, relations):
    buckets, kinds, width = positives.shape[0], relations.shape[0], relations.shape[1]
    if kinds % 2 or buckets % 2 or width % 16:
        raise ValueError("unsupported shapes")
    source, state = source_rows[0, 0], source_state
    target, target_state = target_rows[0, 0], destination_state
    columns, block = source.shape[1], target.shape[1]
    scale = grad_gain / math.sqrt(columns * lax.axis_size("blk") * lax.axis_size("grp"))
    pieces, me = piece_plan()
    me, ids = me[None], relation_ids[:, 0, 0]
    wide, tall = round_up(width, LANES), round_up(width + 1, 8)
    rows = packed_rows(width, kinds, pieces)
    q_pair = [((wide, columns), BF16)] * 2
    sg_pair = [((block, columns), BF16)] * 2
    square = [((wide, wide), F32)]
    moving = [((tall, block), F32)]
    scores = [((block, columns), F32)]
    source_outs = [((width, columns), F32), (source_state.shape, F32)]
    product = 6 * width * width * columns
    updates = buckets // 2
    rel_out, packed_out, y_pair = (relations.shape, F32), ((rows, LANES), F32), [((block, wide), BF16)] * 2
    grads, grads_out = None, ((updates, *relations.shape), F32)
    for update in range(updates):
        bucket, last = 2 * update, update == updates - 1
        if update == 0:
            after, sgh, sgl = call(
                opening_kernel, "opening",
                [me, *(in_hbm(x) for x in (ids, positives, relations, source, target, target_state))], [SMEM] + [HBM] * 6, moving + sg_pair,
                square + q_pair + q_pair + scores + [
                    (relations.shape, F32), (source.shape, F32), (target.shape, F32), (target_state.shape, F32),
                    (positives.shape[1:], jnp.int32), pltpu.SMEM(ids.shape, jnp.int32), pltpu.SemaphoreType.DMA((6,))],
                3 * product)
        else:
            scaled, relations, after, sgh, sgl = call(
                functools.partial(first_kernel, bucket=bucket, pieces=pieces, scale=scale), "first",
                (ids, me, positives, other, relations, *own, xh, xl, target, yh, yl), [SMEM] * 2 + [VMEM] * 10,
                [rel_out, rel_out] + moving + sg_pair, square + q_pair + scores, 3 * product, aliases={5: 0, 6: 1})
        arriving = from_behind(after, "blk", 1)
        args, outs = (ids, relations, source, state, target, sgh, sgl), source_outs + [((width, wide), F32)] + q_pair + q_pair
        if update == 0:
            source, state, grad, qh, ql, xh, xl = call(
                functools.partial(second_kernel, bucket=bucket, place=None), "second",
                args, [SMEM] + [VMEM] * 6, outs, square + q_pair, 4 * product)
        else:
            before = () if grads is None else (grads,)
            source, state, grad, qh, ql, xh, xl, grads = call(
                functools.partial(second_kernel, bucket=bucket, place=update - 1), "second",
                (*args, scaled, *before), [SMEM] + [VMEM] * 7 + [HBM] * len(before), outs + [grads_out],
                square + q_pair + [pltpu.SemaphoreType.DMA((1,))], 4 * product,
                [VMEM] * len(outs) + [HBM], {8: len(outs)} if before else None)
        target = arriving
        packed, sgh, sgl, gh, gl = call(
            functools.partial(third_kernel, bucket=bucket + 1, kinds=kinds, pieces=pieces), "third",
            (ids, me, positives, xh, xl, target, qh, ql, grad), [SMEM] * 2 + [VMEM] * 7,
            [packed_out] + sg_pair + q_pair, scores, 3 * product)

        def close(half, own=None):
            before = tuple(own) if own is not None else () if grads is None else (grads,)
            return call(
                functools.partial(closing_kernel, pieces=pieces, scale=scale, place=updates - 1, half=0 if own is None else 1), "closing",
                (me, half, relations, *before), [SMEM, VMEM, VMEM] + [HBM] * len(before),
                [grads_out, rel_out], [rel_out, rel_out, pltpu.SemaphoreType.DMA((kinds,))],
                product // 4, [HBM, HBM], {3 + i: i for i in range(len(before))})

        own, other, target, source, state, *prepared = sum_everywhere(
            packed,
            lambda *args: call(
                functools.partial(fourth_kernel, bucket=bucket + 1), "fourth",
                (ids, *args), [SMEM] + [VMEM] * len(args), moving + source_outs + ([] if last else q_pair), square, 2 * product),
            (relations, source, state, target, qh, ql, sgh, sgl, gh, gl),
            (lambda target: [target[None, None, :width], target[None, width : width + 1]]) if last else lambda target: call(
                functools.partial(prepare_kernel, width=width), "prepare", (target,), [VMEM], y_pair, (), product // 4),
            close if last else lambda half: call(
                functools.partial(own_kernel, pieces=pieces, scale=scale), "own",
                (me, half, relations), [SMEM, VMEM, VMEM], [rel_out, rel_out], (), product // 4))
        if not last:
            xh, xl, yh, yl = prepared
    grads, relations = close(other, own)
    return (
        source[None, None],
        state,
        *prepared,
        relations,
        grads,
    )


def solution(mesh):
    rows, columns = P("blk", "grp", None, None), P("blk", "grp", None)
    in_specs = (rows, columns, rows, columns, P(None, "blk", "grp", None), P(None, "blk", "grp"), P())
    out_specs = (rows, columns, rows, columns, P(), P())
    return jax.shard_map(shards, mesh=mesh, in_specs=in_specs, out_specs=out_specs, check_vma=False)
```
